32 devices in a mesh: cuts: 4 (over z), dp: 4 (over y, x), mp: 2 (over core).
Axes of the slice: x: 2, y: 2, z: 4, core: 2. Of those that a mesh axis runs over, the one named last changes fastest.
Arguments:
- attn_out: bfloat16 [2048, 3072], P(('cuts', 'dp'), 'mp'), may hold values from -6 to 6
- out_weight: bfloat16 [3072, 6144], P('mp'), may hold values from -0.109375 to 0.109375
- residual: bfloat16 [2048, 6144], P(('cuts', 'dp', 'mp')), may hold values from -45 to 45
- target: bfloat16 [2048, 6144], P(('cuts', 'dp', 'mp')), may hold values from -5 to 5
- norm_gain: float32 [6144], replicated, may hold values from 0.1 to 1.9
Outputs:
- block_out: bfloat16 [2048, 6144], P(('cuts', 'dp', 'mp'))
- attn_grad: bfloat16 [2048, 3072], P(('cuts', 'dp'), 'mp')
- weight_grad: float32 [3072, 6144], P('mp', 'dp')
The draws below stay inside these ranges and needn't reach their ends.
All inputs are finite; a program needn't handle non-finite values.
Results may differ from the reference program's by a relative error of at most 0.018.
Values may be sent and summed in bfloat16 or wider, within the bound.
A program may use at most 128 MiB of HBM per device.

```python
import math
import jax
import jax.numpy as jnp
from jax import lax

D = 6144
TOK_DEV = 128
INNER = 3072
REPLICAS = 16
TOKENS = 2048
N_MP = 2


def draw_residual(key, part):
    key_rows = jax.random.fold_in(key, 11)
    key_cols = jax.random.fold_in(key, 12)
    key_base = jax.random.fold_in(key, 13)
    row_scale = jnp.exp(jax.random.uniform(key_rows, (TOKENS, 1), jnp.float32, math.log(0.3), math.log(3.0)))
    col_scale = jnp.exp(jax.random.uniform(key_cols, (1, D), jnp.float32, math.log(0.3), math.log(3.0)))
    base = jnp.clip(jax.random.normal(key_base, (TOKENS, D), jnp.float32), -5.0, 5.0)
    return (base * row_scale * col_scale).astype(jnp.bfloat16)


def draw_target(key, part):
    key_base = jax.random.fold_in(key, 21)
    key_offset = jax.random.fold_in(key, 22)
    offset = jax.random.uniform(key_offset, (TOKENS, 1), jnp.float32, -1.0, 1.0)
    base = jnp.clip(jax.random.normal(key_base, (TOKENS, D), jnp.float32), -4.0, 4.0)
    return (base + offset).astype(jnp.bfloat16)


def level_of(rng, extent, pieces, least, largest):
    level, own = 1.0, jax.random.fold_in(rng, 6)
    for position, shards_of in pieces:
        draws = jnp.exp(jax.random.uniform(jax.random.fold_in(own, position), (shards_of,), jnp.float32, least / len(pieces), largest / len(pieces)))
        level = level * jnp.repeat(draws, extent[position] // shards_of).reshape([-1 if axis == position else 1 for axis in range(len(extent))])
    return level


def scatter_about(stream_key, shape, width, limit, pieces=(), kind=jnp.bfloat16):
    gain = level_of(stream_key, shape, pieces, -0.22, 0.18) if pieces else 1.0
    array = jax.random.normal(stream_key, shape, jnp.float32) * width * gain
    return jnp.minimum(jnp.maximum(array, -limit), limit).astype(kind)


def setup_inputs(seed: int = 0) -> dict:
    seeds = jax.random.split(jax.random.key(seed), 6)
    return {
        "attn_out": scatter_about(seeds[0], (TOKENS, INNER), 1.0, 6.0, ((0, 16), (1, 2))),
        "out_weight": scatter_about(seeds[1], (INNER, D), INNER ** -0.5, 0.109375, ((0, 2),)),
        "residual": draw_residual(jax.random.fold_in(seeds[5], 71), 0),
        "target": draw_target(jax.random.fold_in(seeds[5], 71), 0),
        "norm_gain": jnp.clip(1.0 + 0.18 * jax.random.normal(seeds[4], (D,), jnp.float32), 0.1, 1.9),
    }


epsilon = 1e-06

def norm_backward(stream, target, norm_gain):
    center = stream - lax.optimization_barrier(jnp.mean(stream, axis=1, keepdims=True))
    inv_std = lax.rsqrt(lax.optimization_barrier(jnp.mean(center * center, axis=1, keepdims=True)) + epsilon)
    normed = center * inv_std
    misfit = normed * norm_gain[None, :] - target.astype(jnp.float32)
    gain_err = misfit * norm_gain[None, :]
    bracket = gain_err - lax.optimization_barrier(jnp.mean(gain_err, axis=1, keepdims=True)) - normed * lax.optimization_barrier(jnp.mean(gain_err * normed, axis=1, keepdims=True))
    return (inv_std * bracket).astype(jnp.bfloat16)

def reference(attn_out, out_weight, residual, target, norm_gain):
    group_cols = INNER // N_MP
    replica_scale = 1.0 / REPLICAS
    heads_all = attn_out.reshape(REPLICAS, TOK_DEV, INNER)
    resid_all = residual.reshape(REPLICAS, TOK_DEV, D)
    target_all = target.reshape(REPLICAS, TOK_DEV, D)

    def replica_step(grad_sum, inputs):
        head_block, resid_block, target_block = inputs
        stream = resid_block.astype(jnp.float32)
        for group_idx in range(N_MP):
            low = group_idx * group_cols
            partial_value = jnp.dot(head_block[:, low:low + group_cols], out_weight[low:low + group_cols], preferred_element_type=jnp.float32)
            stream = stream + lax.optimization_barrier(partial_value.astype(jnp.bfloat16)).astype(jnp.float32)
        cotangent = norm_backward(stream, target_block, norm_gain)
        attn_rows = lax.dot_general(cotangent, out_weight, (((1,), (1,)), ((), ())), preferred_element_type=jnp.float32).astype(jnp.bfloat16)
        shares = lax.dot_general(head_block, cotangent, (((0,), (0,)), ((), ())), preferred_element_type=jnp.float32) * replica_scale
        grad_sum = grad_sum + lax.optimization_barrier(shares.astype(jnp.bfloat16)).astype(jnp.float32)
        return (grad_sum, (stream.astype(jnp.bfloat16), attn_rows))
    grad_sum, outputs = lax.scan(replica_step, jnp.zeros((INNER, D), jnp.float32), (heads_all, resid_all, target_all))
    block_out, attn_grad = outputs
    return (block_out.reshape(TOKENS, D), attn_grad.reshape(TOKENS, INNER), grad_sum)
```

```python
import functools

import jax
import jax.numpy as jnp
from jax import lax
from jax.experimental import pallas as pl
from jax.experimental.pallas import tpu as pltpu
from jax.sharding import PartitionSpec as P

epsilon = 1e-06


def norm_backward(stream, target, norm_gain):
    center = stream - jnp.mean(stream, axis=1, keepdims=True)
    inv_std = lax.rsqrt(jnp.mean(center * center, axis=1, keepdims=True) + epsilon)
    normed = center * inv_std
    misfit = normed * norm_gain[None, :] - target.astype(jnp.float32)
    gain_err = misfit * norm_gain[None, :]
    bracket = (
        gain_err
        - jnp.mean(gain_err, axis=1, keepdims=True)
        - normed * jnp.mean(gain_err * normed, axis=1, keepdims=True)
    )
    return (inv_std * bracket).astype(jnp.bfloat16)


def per_device(attn_out, out_weight, residual, target, norm_gain):
    tokens_dev = attn_out.shape[0]
    head_cols = attn_out.shape[1]
    replica_scale = 1.0 / (lax.axis_size("cuts") * lax.axis_size("dp"))
    summed = lax.psum_scatter(
        jnp.dot(attn_out, out_weight, preferred_element_type=jnp.float32).astype(jnp.bfloat16),
        "mp",
        scatter_dimension=0,
        tiled=True,
    ).astype(jnp.float32)
    stream = summed + residual.astype(jnp.float32)
    block_out = stream.astype(jnp.bfloat16)
    cotangent = norm_backward(stream, target, norm_gain)
    portion = lax.all_gather(cotangent, "mp", axis=0, tiled=True)
    stored = portion
    act_acc = lax.dot_general(
        portion, out_weight, (((1,), (1,)), ((), ())), preferred_element_type=jnp.float32
    )
    collected, act_acc = (stored, act_acc)
    attn_grad = act_acc.astype(jnp.bfloat16)
    columns = lax.all_to_all(collected, "dp", split_axis=1, concat_axis=0, tiled=True)
    column_width = columns.shape[1]
    portion = lax.all_gather(attn_out, "dp", axis=0, tiled=True)
    blocks_in = portion.shape[0] // tokens_dev
    head_block = portion.reshape(blocks_in, tokens_dev, head_cols)
    column_part = columns.reshape(blocks_in, tokens_dev, column_width)
    shares = (
        jnp.einsum("bti,btj->bij", head_block, column_part, preferred_element_type=jnp.float32)
        * replica_scale
    )
    rounded = lax.optimization_barrier(shares.astype(jnp.bfloat16))
    grad_block = jnp.sum(rounded.astype(jnp.float32), axis=0)
    weight_grad = lax.psum(grad_block.astype(jnp.bfloat16), "cuts").astype(jnp.float32)
    return (block_out, attn_grad, weight_grad)


NS = jax.named_scope
MESH = pl.DeviceIdType.MESH


def remote(src, dst, send_sem, recv_sem, **where):
    return pltpu.make_async_remote_copy(
        src_ref=src, dst_ref=dst, send_sem=send_sem, recv_sem=recv_sem, device_id=where, device_id_type=MESH
    )


def last_plane(nz, z):
    return jnp.where(2 * z < nz - 1, nz - 1, 0)


def fused(
    nz, ndp, chunk, attn_h, w_h, res_h, tgt_h, gain_h, blk_v, agrad_v, acc, a_v, cot_v,
    w_v, rows_v, part, part_in, res_v, tgt_v, gain_v,
    ld_s, w_s, p_s, p_r, au_s, ad_s, az_r, ax_s, ax_r, ay_s, ay_r, rx_s, rx_r, ry_s, ry_r,
    cp_s, cq_s, cq_r, cu_s, cd_s, c_r, ce_s, ce_r,
):
    z, dp, m = lax.axis_index("cuts"), lax.axis_index("dp"), lax.axis_index("mp")
    other = 1 - m
    px, py = lax.rem(dp, 2), lax.div(dp, 2)
    xn, yn, dg = 2 * py + 1 - px, 2 * (1 - py) + px, 2 * (1 - py) + 1 - px
    peers = (dp, xn, yn, dg)
    tok, heads = attn_h.shape
    half, width = res_h.shape
    cols = width // ndp
    chunks = width // chunk
    has_up, has_down = z + 1 < nz, z >= 1

    a_load = pltpu.make_async_copy(attn_h, a_v.at[z, dp], ld_s.at[0])
    loads = [
        pltpu.make_async_copy(res_h, res_v, ld_s.at[1]),
        pltpu.make_async_copy(tgt_h, tgt_v, ld_s.at[2]),
        pltpu.make_async_copy(gain_h, gain_v, ld_s.at[3]),
    ]
    a_load.start()

    def w_load(c):
        at = pl.ds(pl.multiple_of(c * chunk, chunk), chunk)
        return pltpu.make_async_copy(w_h.at[:, at], w_v.at[:, at], w_s.at[c])

    barrier = pltpu.get_barrier_semaphore()
    pl.semaphore_signal(barrier, inc=1, device_id={"mp": other}, device_id_type=MESH)
    for peer in peers[1:]:
        pl.semaphore_signal(barrier, inc=1, device_id={"dp": peer}, device_id_type=MESH)

    @pl.when(has_up)
    def _():
        pl.semaphore_signal(barrier, inc=1, device_id={"cuts": z + 1}, device_id_type=MESH)

    @pl.when(has_down)
    def _():
        pl.semaphore_signal(barrier, inc=1, device_id={"cuts": z - 1}, device_id_type=MESH)

    with NS("aload"):
        a_load.wait()
    for c in range(chunks):
        w_load(c).start()
    for load in loads:
        load.start()
    with NS("barrier"):
        pl.semaphore_wait(barrier, ndp + jnp.where(has_up, 1, 0) + jnp.where(has_down, 1, 0))

    def rows(h):
        return pl.ds(h * half, half)

    def piece(l, d, h):
        return a_v.at[l, d, rows(h)]

    def a_up(l, h):
        return remote(piece(l, dp, h), piece(l, dp, h), au_s.at[l, h], az_r.at[l, h], cuts=z + 1)

    def a_down(l, h):
        return remote(piece(l, dp, h), piece(l, dp, h), ad_s.at[l, h], az_r.at[l, h], cuts=z - 1)

    def a_x(l, h):
        return remote(piece(l, dp, h), piece(l, dp, h), ax_s.at[l, h], ax_r.at[l, h], dp=xn)

    def a_y(l, h):
        return remote(piece(l, dp, h), piece(l, dp, h), ay_s.at[l, h], ay_r.at[l, h], dp=yn)

    def a_x_in(l, h):
        return remote(piece(l, xn, h), piece(l, xn, h), ax_s.at[l, h], ax_r.at[l, h], dp=xn)

    def a_y_in(l, h):
        return remote(piece(l, yn, h), piece(l, yn, h), ay_s.at[l, h], ay_r.at[l, h], dp=yn)

    def r_y(l):
        return remote(piece(l, xn, 0), piece(l, xn, 0), ry_s.at[l], ry_r.at[l], dp=yn)

    def r_x(l):
        return remote(piece(l, yn, 1), piece(l, yn, 1), rx_s.at[l], rx_r.at[l], dp=xn)

    def r_y_in(l):
        return remote(piece(l, dg, 0), piece(l, dg, 0), ry_s.at[l], ry_r.at[l], dp=yn)

    def r_x_in(l):
        return remote(piece(l, dg, 1), piece(l, dg, 1), rx_s.at[l], rx_r.at[l], dp=xn)

    def c_up(l, d, src=None):
        return remote(cot_v.at[l, d, m] if src is None else src, cot_v.at[l, d, m], cu_s.at[l, d], c_r.at[l, d], cuts=z + 1)

    def c_down(l, d, src=None):
        return remote(cot_v.at[l, d, m] if src is None else src, cot_v.at[l, d, m], cd_s.at[l, d], c_r.at[l, d], cuts=z - 1)

    def c_pair(l, d):
        return remote(cot_v.at[l, d, m], cot_v.at[l, d, m], ce_s.at[l, d], ce_r.at[l, d], mp=other)

    def c_pair_in(l, d):
        return remote(cot_v.at[l, d, other], cot_v.at[l, d, other], ce_s.at[l, d], ce_r.at[l, d], mp=other)

    def both(k, f):
        pl.when(z - k >= 0)(lambda: f(z - k))
        pl.when(z + k < nz)(lambda: f(z + k))

    def a_hop(k, h):
        if k >= nz:
            return

        @pl.when(z - k >= 0)
        def _():
            with NS("ahop"):
                a_up(z - k, h).wait_recv()
            pl.when(has_up)(lambda: a_up(z - k, h).start())

        @pl.when(z + k < nz)
        def _():
            with NS("ahop"):
                a_down(z + k, h).wait_recv()
            pl.when(has_down)(lambda: a_down(z + k, h).start())

    def a_plane(l):
        a_x(l, 0).start()
        a_y(l, 1).start()
        a_x(l, 1).start()
        a_y(l, 0).start()

    def relay(l):
        with NS("relay"):
            a_x_in(l, 0).wait_recv()
        r_y(l).start()
        with NS("relay"):
            a_y_in(l, 1).wait_recv()
        r_x(l).start()

    for h in range(2):
        pl.when(has_up)(lambda: a_up(z, h).start())
        pl.when(has_down)(lambda: a_down(z, h).start())
    a_plane(z)

    def p_send(c):
        at = pl.ds(pl.multiple_of(c * chunk, chunk), chunk)
        return remote(part.at[other, :, at], part_in.at[:, at], p_s.at[c], p_r.at[c], mp=other)

    @pl.loop(0, chunks)
    def _(c):
        at = pl.ds(pl.multiple_of(c * chunk, chunk), chunk)
        with NS("wload"):
            w_load(c).wait()
        value = jnp.dot(a_v[z, dp], w_v[:, at], preferred_element_type=jnp.float32).astype(jnp.bfloat16)
        part[0, :, at] = value[:half]
        part[1, :, at] = value[half:]
        p_send(c).start()

    a_hop(1, 0)
    relay(z)
    with NS("loads"):
        for load in loads:
            load.wait()

    with NS("psend"):

        @pl.loop(0, chunks)
        def _(c):
            p_send(c).wait()

    step = 16
    gain = gain_v[...]

    @pl.loop(0, half // step)
    def _(i):
        at = pl.ds(pl.multiple_of(i * step, step), step)
        stream = (
            part[m, at, :].astype(jnp.float32) + part_in[at, :].astype(jnp.float32) + res_v[at, :].astype(jnp.float32)
        )
        blk_v[at, :] = stream.astype(jnp.bfloat16)
        center = stream - jnp.mean(stream, axis=1, keepdims=True)
        inv_std = lax.rsqrt(jnp.mean(center * center, axis=1, keepdims=True) + epsilon)
        normed = center * inv_std
        gain_err = (normed * gain - tgt_v[at, :].astype(jnp.float32)) * gain
        bracket = (
            gain_err
            - jnp.mean(gain_err, axis=1, keepdims=True)
            - normed * jnp.mean(gain_err * normed, axis=1, keepdims=True)
        )
        cot = (inv_std * bracket).astype(jnp.bfloat16)
        for d in range(ndp):
            rows_v[d, m, at, :] = cot[:, d * cols : (d + 1) * cols]

    def c_plane(k):
        return remote(rows_v.at[peers[k], m], cot_v.at[z, dp, m], cp_s.at[k], c_r.at[z, dp], dp=peers[k])

    def c_rows():
        return remote(rows_v.at[:, m], rows_v.at[:, m], cq_s.at[0], cq_r.at[0], mp=other)

    def c_rows_in():
        return remote(rows_v.at[:, other], rows_v.at[:, other], cq_s.at[0], cq_r.at[0], mp=other)

    own = rows_v.at[dp, m]
    pl.when(has_up)(lambda: c_up(z, dp, own).start())
    pl.when(has_down)(lambda: c_down(z, dp, own).start())
    for k in range(1, ndp):
        c_plane(k).start()
    c_rows().start()
    cot_v[z, dp, m] = rows_v[dp, m]

    a_hop(1, 1)
    both(1, a_plane)
    with NS("crows"):
        c_rows_in().wait_recv()
    cot_v[z, dp, other] = rows_v[dp, other]

    tile = 512 if heads % 512 == 0 else heads

    def attn_tile(j):
        at = slice(j * tile, (j + 1) * tile)
        total = jnp.zeros((tok, tile), jnp.float32)
        for d in range(ndp):
            total += lax.dot_general(
                rows_v[d].reshape(tok, cols), w_v[at, d * cols : (d + 1) * cols], (((1,), (1,)), ((), ())),
                preferred_element_type=jnp.float32,
            )
        agrad_v[:, at] = total.astype(jnp.bfloat16)

    def c_forward(l, d, up, down):
        pl.when(up)(lambda: c_up(l, d).start())
        pl.when(down)(lambda: c_down(l, d).start())
        c_pair(l, d).start()

    tiles = heads // tile
    for j in range(tiles):
        attn_tile(j)
        if j < 2:
            a_hop(2, j)
    for h in range(tiles, 2):
        a_hop(2, h)
    both(2, a_plane)
    for k in range(1, ndp):
        with NS("cplane"):
            c_up(z, peers[k]).wait_recv()
        c_forward(z, peers[k], has_up, has_down)

    wide = 256 if heads % 256 == 0 else heads

    def accumulate(l, first, count, fresh):
        @pl.loop(0, heads // wide)
        def _(j):
            at = pl.ds(pl.multiple_of(j * wide, wide), wide)
            value = lax.dot_general(
                a_v[l, pl.ds(first, count), :, at].reshape(count * tok, wide),
                cot_v[l, pl.ds(first, count)].reshape(count * tok, cols),
                (((0,), (0,)), ((), ())),
                preferred_element_type=jnp.float32,
            )
            acc[at, :] = value if fresh else acc[at, :] + value

    def a_arrived(l):
        a_x_in(l, 1).wait_recv()
        a_y_in(l, 0).wait_recv()
        r_y_in(l).wait_recv()
        r_x_in(l).wait_recv()

    with NS("cpair0"):
        for k in range(1, ndp):
            c_pair_in(z, peers[k]).wait_recv()
    with NS("aarr0"):
        a_arrived(z)
    with NS("group0"):
        accumulate(z, 0, ndp, True)

    both(1, relay)
    last = last_plane(nz, z)
    for k in range(1, nz):
        for h in range(2):
            a_hop(k + 2, h)
        if k + 2 < nz:
            both(k + 2, a_plane)
        for j in range(ndp):

            @pl.when(z - k >= 0)
            def _():
                with NS("cup"):
                    c_up(z - k, peers[j]).wait_recv()
                c_forward(z - k, peers[j], has_up, False)

            @pl.when(z + k < nz)
            def _():
                with NS("cdown"):
                    c_down(z + k, peers[j]).wait_recv()
                c_forward(z + k, peers[j], False, has_down)

            if j == 1 and k + 1 < nz:
                both(k + 1, relay)

            def near(l):
                for i in range(2):
                    c_pair_in(l, peers[i]).wait_recv()
                a_x_in(l, 1).wait_recv()
                accumulate(l, 2 * py, 2, False)

            if j == 2:
                both(k, lambda l: pl.when(l == last)(lambda: near(l)))

        def finish(l):
            with NS("cpair"):

                @pl.when(l == last)
                def _():
                    for j in range(2, ndp):
                        c_pair_in(l, peers[j]).wait_recv()
                    a_y_in(l, 0).wait_recv()
                    r_y_in(l).wait_recv()
                    r_x_in(l).wait_recv()

                @pl.when(l != last)
                def _():
                    for j in range(ndp):
                        c_pair_in(l, peers[j]).wait_recv()
                    a_arrived(l)

            @pl.when(l != last)
            def _():
                with NS("group"):
                    accumulate(l, 0, ndp, False)

        both(k, finish)

    @pl.loop(0, nz)
    def _(l):
        @pl.when(has_up & (l <= z))
        def _():
            for h in range(2):
                a_up(l, h).wait_send()
            for d in range(ndp):
                c_up(l, d).wait_send()

        @pl.when(has_down & (l >= z))
        def _():
            for h in range(2):
                a_down(l, h).wait_send()
            for d in range(ndp):
                c_down(l, d).wait_send()

        for h in range(2):
            a_x(l, h).wait_send()
            a_y(l, h).wait_send()
        r_x(l).wait_send()
        r_y(l).wait_send()
        for k in range(1, ndp):
            c_pair(l, peers[k]).wait_send()

        @pl.when(l != z)
        def _():
            c_pair(l, dp).wait_send()

    for k in range(1, ndp):
        c_plane(k).wait_send()
    c_rows().wait_send()


def finishing(nz, ndp, blk_i, agrad_i, acc, a_v, cot_v, blk_o, agrad_o, wgrad_o, out_v, s, o_s):
    z, dp = lax.axis_index("cuts"), lax.axis_index("dp")
    last = last_plane(nz, z)
    first = 2 * (1 - lax.div(dp, 2))
    tok, heads = agrad_i.shape
    cols = acc.shape[1]
    scale = 1.0 / (nz * ndp)
    blk_copy = pltpu.make_async_copy(blk_i, blk_o, s.at[0])
    agrad_copy = pltpu.make_async_copy(agrad_i, agrad_o, s.at[1])
    blk_copy.start()
    agrad_copy.start()
    wide = 256 if heads % 256 == 0 else heads

    def out_copy(j):
        at = pl.ds(pl.multiple_of(j * wide, wide), wide)
        return pltpu.make_async_copy(out_v.at[at, :], wgrad_o.at[at, :], o_s.at[j])

    @pl.loop(0, heads // wide)
    def _(j):
        at = pl.ds(pl.multiple_of(j * wide, wide), wide)
        value = lax.dot_general(
            a_v[last, pl.ds(first, 2), :, at].reshape(2 * tok, wide),
            cot_v[last, pl.ds(first, 2)].reshape(2 * tok, cols),
            (((0,), (0,)), ((), ())),
            preferred_element_type=jnp.float32,
        )
        out_v[at, :] = scale * (acc[at, :] + value)
        out_copy(j).start()

    blk_copy.wait()
    agrad_copy.wait()

    @pl.loop(0, heads // wide)
    def _(j):
        out_copy(j).wait()


def fused_device(nz, ndp, attn_out, out_weight, residual, target, norm_gain):
    tok, heads = attn_out.shape
    half, width = residual.shape
    cols = width // ndp
    chunk = 512 if width % 512 == 0 else 128
    chunks = width // chunk
    tiles = heads // 256 if heads % 256 == 0 else 1
    bf16, f32 = jnp.bfloat16, jnp.float32
    dma = pltpu.SemaphoreType.DMA
    in_vmem = pl.BlockSpec(memory_space=pltpu.VMEM)
    in_hbm = pl.BlockSpec(memory_space=pl.ANY)
    args = [attn_out, out_weight, residual, target, norm_gain.reshape(1, width)]
    args = [pltpu.with_memory_space_constraint(arg, pltpu.HBM) for arg in args]
    kept = pl.pallas_call(
        functools.partial(fused, nz, ndp, chunk),
        out_shape=(
            pltpu.VMEM((half, width), bf16),
            pltpu.VMEM((tok, heads), bf16),
            pltpu.VMEM((heads, cols), f32),
            pltpu.VMEM((nz, ndp, tok, heads), bf16),
            pltpu.VMEM((nz, ndp, 2, half, cols), bf16),
        ),
        in_specs=[in_hbm] * 5,
        out_specs=(in_vmem,) * 5,
        scratch_shapes=[
            pltpu.VMEM((heads, width), bf16),
            pltpu.VMEM((ndp, 2, half, cols), bf16),
            pltpu.VMEM((2, half, width), bf16),
            pltpu.VMEM((half, width), bf16),
            pltpu.VMEM((half, width), bf16),
            pltpu.VMEM((half, width), bf16),
            pltpu.VMEM((1, width), f32),
            dma((4,)), dma((chunks,)), dma((chunks,)), dma((chunks,)),
            dma((nz, 2)), dma((nz, 2)), dma((nz, 2)),
            dma((nz, 2)), dma((nz, 2)), dma((nz, 2)), dma((nz, 2)),
            dma((nz,)), dma((nz,)), dma((nz,)), dma((nz,)),
            dma((ndp,)), dma((1,)), dma((1,)),
            dma((nz, ndp)), dma((nz, ndp)), dma((nz, ndp)), dma((nz, ndp)), dma((nz, ndp)),
        ],
        compiler_params=pltpu.CompilerParams(
            collective_id=0, has_side_effects=True, vmem_limit_bytes=34 * 1000 * 1000
        ),
    )(*args)
    return pl.pallas_call(
        functools.partial(finishing, nz, ndp),
        out_shape=(
            jax.ShapeDtypeStruct((half, width), bf16),
            jax.ShapeDtypeStruct((tok, heads), bf16),
            jax.ShapeDtypeStruct((heads, cols), f32),
        ),
        in_specs=[in_vmem] * 5,
        out_specs=(in_hbm,) * 3,
        scratch_shapes=[pltpu.VMEM((heads, cols), f32), dma((2,)), dma((tiles,))],
        compiler_params=pltpu.CompilerParams(vmem_limit_bytes=16 * 1000 * 1000),
    )(*kept)


def solution(mesh):
    if mesh.shape["mp"] == 2 and mesh.shape["dp"] == 4 and mesh.shape["cuts"] > 1:
        body = functools.partial(fused_device, mesh.shape["cuts"], mesh.shape["dp"])
    else:
        body = per_device
    placed = (
        P(("cuts", "dp"), "mp"),
        P("mp", None),
        P(("cuts", "dp", "mp"), None),
        P(("cuts", "dp", "mp"), None),
        P(),
    )
    return jax.shard_map(
        body,
        mesh=mesh,
        in_specs=placed,
        out_specs=(P(("cuts", "dp", "mp"), None), P(("cuts", "dp"), "mp"), P("mp", "dp")),
        check_vma=False,
    )
```

```python
import functools

import jax
import jax.numpy as jnp
from jax import lax
from jax.experimental import pallas as pl
from jax.experimental.pallas import tpu as pltpu
from jax.sharding import PartitionSpec as P

epsilon = 1e-06


def norm_backward(stream, target, norm_gain):
    center = stream - jnp.mean(stream, axis=1, keepdims=True)
    inv_std = lax.rsqrt(jnp.mean(center * center, axis=1, keepdims=True) + epsilon)
    normed = center * inv_std
    misfit = normed * norm_gain[None, :] - target.astype(jnp.float32)
    gain_err = misfit * norm_gain[None, :]
    bracket = (
        gain_err
        - jnp.mean(gain_err, axis=1, keepdims=True)
        - normed * jnp.mean(gain_err * normed, axis=1, keepdims=True)
    )
    return (inv_std * bracket).astype(jnp.bfloat16)


def per_device(attn_out, out_weight, residual, target, norm_gain):
    tokens_dev = attn_out.shape[0]
    head_cols = attn_out.shape[1]
    replica_scale = 1.0 / (lax.axis_size("cuts") * lax.axis_size("dp"))
    summed = lax.psum_scatter(
        jnp.dot(attn_out, out_weight, preferred_element_type=jnp.float32).astype(jnp.bfloat16),
        "mp",
        scatter_dimension=0,
        tiled=True,
    ).astype(jnp.float32)
    stream = summed + residual.astype(jnp.float32)
    block_out = stream.astype(jnp.bfloat16)
    cotangent = norm_backward(stream, target, norm_gain)
    portion = lax.all_gather(cotangent, "mp", axis=0, tiled=True)
    stored = portion
    act_acc = lax.dot_general(
        portion, out_weight, (((1,), (1,)), ((), ())), preferred_element_type=jnp.float32
    )
    collected, act_acc = (stored, act_acc)
    attn_grad = act_acc.astype(jnp.bfloat16)
    columns = lax.all_to_all(collected, "dp", split_axis=1, concat_axis=0, tiled=True)
    column_width = columns.shape[1]
    portion = lax.all_gather(attn_out, "dp", axis=0, tiled=True)
    blocks_in = portion.shape[0] // tokens_dev
    head_block = portion.reshape(blocks_in, tokens_dev, head_cols)
    column_part = columns.reshape(blocks_in, tokens_dev, column_width)
    shares = (
        jnp.einsum("bti,btj->bij", head_block, column_part, preferred_element_type=jnp.float32)
        * replica_scale
    )
    rounded = lax.optimization_barrier(shares.astype(jnp.bfloat16))
    grad_block = jnp.sum(rounded.astype(jnp.float32), axis=0)
    weight_grad = lax.psum(grad_block.astype(jnp.bfloat16), "cuts").astype(jnp.float32)
    return (block_out, attn_grad, weight_grad)


NS = jax.named_scope
MESH = pl.DeviceIdType.MESH


def remote(src, dst, send_sem, recv_sem, **where):
    return pltpu.make_async_remote_copy(
        src_ref=src, dst_ref=dst, send_sem=send_sem, recv_sem=recv_sem, device_id=where, device_id_type=MESH
    )


def last_plane(nz, z):
    return jnp.where(2 * z < nz - 1, nz - 1, 0)


def fused(
    nz, ndp, chunk, attn_h, w_h, res_h, tgt_h, gain_h, blk_v, agrad_v, acc, a_v, cot_v,
    w_v, rows_v, part, part_in, res_v, tgt_v, gain_v,
    ld_s, w_s, p_s, p_r, up_s, dn_s, az_r, pl_s, fx_r, fy_r, pl_r, cp_s, cq_s, cq_r, c_r, ce_s, ce_r,
):
    z, dp, m = lax.axis_index("cuts"), lax.axis_index("dp"), lax.axis_index("mp")
    other = 1 - m
    px, py = lax.rem(dp, 2), lax.div(dp, 2)
    xn, yn, dg = 2 * py + 1 - px, 2 * (1 - py) + px, 2 * (1 - py) + 1 - px
    peers = (dp, xn, yn, dg)
    tok, heads = attn_h.shape
    half, width = res_h.shape
    cols = width // ndp
    chunks = width // chunk
    per_load = 2 if chunks % 2 == 0 else 1
    last = last_plane(nz, z)
    has_up, has_down = z + 1 < nz, z >= 1

    a_load = pltpu.make_async_copy(attn_h, a_v.at[z, dp], ld_s.at[0])
    loads = [
        pltpu.make_async_copy(res_h, res_v, ld_s.at[1]),
        pltpu.make_async_copy(tgt_h, tgt_v, ld_s.at[1]),
        pltpu.make_async_copy(gain_h, gain_v, ld_s.at[2]),
    ]
    a_load.start()

    def w_load(c):
        at = pl.ds(pl.multiple_of(c * per_load * chunk, chunk), per_load * chunk)
        return pltpu.make_async_copy(w_h.at[:, at], w_v.at[:, at], w_s.at[c])

    barrier = pltpu.get_barrier_semaphore()
    pl.semaphore_signal(barrier, inc=1, device_id={"mp": other}, device_id_type=MESH)
    for peer in peers[1:]:
        pl.semaphore_signal(barrier, inc=1, device_id={"dp": peer}, device_id_type=MESH)

    @pl.when(has_up)
    def _():
        pl.semaphore_signal(barrier, inc=1, device_id={"cuts": z + 1}, device_id_type=MESH)

    @pl.when(has_down)
    def _():
        pl.semaphore_signal(barrier, inc=1, device_id={"cuts": z - 1}, device_id_type=MESH)

    with NS("aload"):
        a_load.wait()
    for c in range(chunks // per_load):
        w_load(c).start()
    for load in loads:
        load.start()
    with NS("barrier"):
        pl.semaphore_wait(barrier, ndp + jnp.where(has_up, 1, 0) + jnp.where(has_down, 1, 0))

    def rows(h):
        return pl.ds(h * half, half)

    def piece(l, d, h):
        return a_v.at[l, d, rows(h)]

    def a_up(l, h):
        return remote(piece(l, dp, h), piece(l, dp, h), up_s.at[l], az_r.at[l, h], cuts=z + 1)

    def a_down(l, h):
        return remote(piece(l, dp, h), piece(l, dp, h), dn_s.at[l], az_r.at[l, h], cuts=z - 1)

    def a_x(l, h):
        return remote(piece(l, dp, h), piece(l, dp, h), pl_s.at[l], (fx_r if h == 0 else pl_r).at[l], dp=xn)

    def a_y(l, h):
        return remote(piece(l, dp, h), piece(l, dp, h), pl_s.at[l], (fy_r if h == 1 else pl_r).at[l], dp=yn)

    def first_x_in(l):
        return remote(piece(l, xn, 0), piece(l, xn, 0), pl_s.at[l], fx_r.at[l], dp=xn)

    def first_y_in(l):
        return remote(piece(l, yn, 1), piece(l, yn, 1), pl_s.at[l], fy_r.at[l], dp=yn)

    def r_y(l):
        return remote(piece(l, xn, 0), piece(l, xn, 0), pl_s.at[l], pl_r.at[l], dp=yn)

    def r_x(l):
        return remote(piece(l, yn, 1), piece(l, yn, 1), pl_s.at[l], pl_r.at[l], dp=xn)

    def rest_in(l):
        return remote(a_v.at[l, :2], a_v.at[l, :2], pl_s.at[l], pl_r.at[l], dp=xn)

    def sent_up(l):
        return remote(a_v.at[l, :3], a_v.at[l, :3], up_s.at[l], pl_r.at[l], cuts=z + 1)

    def sent_down(l):
        return remote(a_v.at[l, :3], a_v.at[l, :3], dn_s.at[l], pl_r.at[l], cuts=z - 1)

    def sent_plane(l):
        return remote(a_v.at[l, :3], a_v.at[l, :3], pl_s.at[l], pl_r.at[l], dp=xn)

    def c_up(l, d, src=None):
        return remote(cot_v.at[l, d, m] if src is None else src, cot_v.at[l, d, m], up_s.at[l], c_r.at[l, d], cuts=z + 1)

    def c_down(l, d, src=None):
        return remote(cot_v.at[l, d, m] if src is None else src, cot_v.at[l, d, m], dn_s.at[l], c_r.at[l, d], cuts=z - 1)

    def c_pair(l, d, group):
        return remote(cot_v.at[l, d, m], cot_v.at[l, d, m], ce_s.at[l], ce_r.at[group], mp=other)

    def c_pairs(l, count, group):
        blocks = cot_v.at[l, :count, other]
        return remote(blocks, blocks, ce_s.at[l], ce_r.at[group], mp=other)

    def both(k, f):
        pl.when(z - k >= 0)(lambda: f(z - k))
        pl.when(z + k < nz)(lambda: f(z + k))

    def a_hop(k, h):
        if k >= nz:
            return

        @pl.when(z - k >= 0)
        def _():
            with NS("ahop"):
                a_up(z - k, h).wait_recv()
            pl.when(has_up)(lambda: a_up(z - k, h).start())

        @pl.when(z + k < nz)
        def _():
            with NS("ahop"):
                a_down(z + k, h).wait_recv()
            pl.when(has_down)(lambda: a_down(z + k, h).start())

    def a_plane(l):
        a_x(l, 0).start()
        a_y(l, 1).start()
        a_x(l, 1).start()
        a_y(l, 0).start()

    def relay(l):
        with NS("relay"):
            first_x_in(l).wait_recv()
        r_y(l).start()
        with NS("relay"):
            first_y_in(l).wait_recv()
        r_x(l).start()

    for h in range(2):
        pl.when(has_up)(lambda: a_up(z, h).start())
        pl.when(has_down)(lambda: a_down(z, h).start())
    a_plane(z)

    def p_send(c):
        at = pl.ds(pl.multiple_of(c * chunk, chunk), chunk)
        return remote(part.at[other, :, at], part_in.at[:, at], p_s.at[0], p_r.at[0], mp=other)

    @pl.loop(0, chunks)
    def _(c):
        at = pl.ds(pl.multiple_of(c * chunk, chunk), chunk)
        pl.when(lax.rem(c, per_load) == 0)(lambda: w_load(lax.div(c, per_load)).wait())
        value = jnp.dot(a_v[z, dp], w_v[:, at], preferred_element_type=jnp.float32).astype(jnp.bfloat16)
        part[0, :, at] = value[:half]
        part[1, :, at] = value[half:]
        p_send(c).start()

    a_hop(1, 0)
    relay(z)
    with NS("loads"):
        pltpu.make_async_copy(part, part, ld_s.at[1]).wait()
        loads[2].wait()

    with NS("psend"):
        remote(part_in, part_in, p_s.at[0], p_r.at[0], mp=other).wait()

    step = 16
    gain = gain_v[...]

    @pl.loop(0, half // step)
    def _(i):
        at = pl.ds(pl.multiple_of(i * step, step), step)
        stream = (
            part[m, at, :].astype(jnp.float32) + part_in[at, :].astype(jnp.float32) + res_v[at, :].astype(jnp.float32)
        )
        blk_v[at, :] = stream.astype(jnp.bfloat16)
        center = stream - jnp.mean(stream, axis=1, keepdims=True)
        inv_std = lax.rsqrt(jnp.mean(center * center, axis=1, keepdims=True) + epsilon)
        normed = center * inv_std
        gain_err = (normed * gain - tgt_v[at, :].astype(jnp.float32)) * gain
        bracket = (
            gain_err
            - jnp.mean(gain_err, axis=1, keepdims=True)
            - normed * jnp.mean(gain_err * normed, axis=1, keepdims=True)
        )
        cot = (inv_std * bracket).astype(jnp.bfloat16)
        for d in range(ndp):
            rows_v[d, m, at, :] = cot[:, d * cols : (d + 1) * cols]

    def c_plane(k):
        return remote(rows_v.at[peers[k], m], cot_v.at[z, dp, m], cp_s.at[0], c_r.at[z, dp], dp=peers[k])

    def c_rows():
        return remote(rows_v.at[:, m], rows_v.at[:, m], cq_s.at[0], cq_r.at[0], mp=other)

    def c_rows_in():
        return remote(rows_v.at[:, other], rows_v.at[:, other], cq_s.at[0], cq_r.at[0], mp=other)

    own = rows_v.at[dp, m]
    pl.when(has_up)(lambda: c_up(z, dp, own).start())
    pl.when(has_down)(lambda: c_down(z, dp, own).start())
    for k in range(1, ndp):
        c_plane(k).start()
    c_rows().start()
    cot_v[z, dp, m] = rows_v[dp, m]

    a_hop(1, 1)
    both(1, a_plane)
    with NS("crows"):
        c_rows_in().wait_recv()
    cot_v[z, dp, other] = rows_v[dp, other]

    tile = 512 if heads % 512 == 0 else heads

    def attn_tile(j):
        at = slice(j * tile, (j + 1) * tile)
        total = jnp.zeros((tok, tile), jnp.float32)
        for d in range(ndp):
            total += lax.dot_general(
                rows_v[d].reshape(tok, cols), w_v[at, d * cols : (d + 1) * cols], (((1,), (1,)), ((), ())),
                preferred_element_type=jnp.float32,
            )
        agrad_v[:, at] = total.astype(jnp.bfloat16)

    def c_forward(l, j, up, down):
        pl.when(up)(lambda: c_up(l, peers[j]).start())
        pl.when(down)(lambda: c_down(l, peers[j]).start())
        c_pair(l, peers[j], l if j < 2 else jnp.where(l == last, nz, l)).start()

    tiles = heads // tile
    for j in range(tiles):
        attn_tile(j)
        if j < 2:
            a_hop(2, j)
    for h in range(tiles, 2):
        a_hop(2, h)
    both(2, a_plane)
    for k in range(1, ndp):
        with NS("cplane"):
            c_up(z, peers[k]).wait_recv()
        c_forward(z, k, has_up, has_down)

    wide = 256 if heads % 256 == 0 else heads

    def accumulate(l, first, count, fresh):
        @pl.loop(0, heads // wide)
        def _(j):
            at = pl.ds(pl.multiple_of(j * wide, wide), wide)
            value = lax.dot_general(
                a_v[l, pl.ds(first, count), :, at].reshape(count * tok, wide),
                cot_v[l, pl.ds(first, count)].reshape(count * tok, cols),
                (((0,), (0,)), ((), ())),
                preferred_element_type=jnp.float32,
            )
            acc[at, :] = value if fresh else acc[at, :] + value

    with NS("cpair0"):
        c_pairs(z, ndp - 1, z).wait_recv()
    with NS("aarr0"):
        rest_in(z).wait_recv()
    with NS("group0"):
        accumulate(z, 0, ndp, True)

    def drain():
        @pl.loop(0, nz)
        def _(l):
            pl.when(has_up & (l <= z))(lambda: sent_up(l).wait_send())
            pl.when(has_down & (l >= z))(lambda: sent_down(l).wait_send())
            sent_plane(l).wait_send()

            @pl.when((l != last) & (l != z))
            def _():
                c_pairs(l, ndp, l).wait_send()

        c_pairs(z, ndp - 1, z).wait_send()
        blocks = cot_v.at[z, : ndp - 1, m]
        remote(blocks, blocks, cp_s.at[0], c_r.at[z, dp], dp=xn).wait_send()
        c_rows().wait_send()

    both(1, relay)
    for k in range(1, nz):
        if k == nz - 1:
            with NS("drain"):
                drain()
        for h in range(2):
            a_hop(k + 2, h)
        if k + 2 < nz:
            both(k + 2, a_plane)
        for j in range(ndp):

            @pl.when(z - k >= 0)
            def _():
                with NS("cup"):
                    c_up(z - k, peers[j]).wait_recv()
                c_forward(z - k, j, has_up, False)

            @pl.when(z + k < nz)
            def _():
                with NS("cdown"):
                    c_down(z + k, peers[j]).wait_recv()
                c_forward(z + k, j, False, has_down)

            if j == 1 and k + 1 < nz:
                both(k + 1, relay)

            def near(l):
                c_pairs(l, 2, l).wait_recv()
                rest_in(l).wait_recv()
                with NS("near"):
                    accumulate(l, 2 * py, 2, False)

            if j == 1:
                both(k, lambda l: pl.when(l == last)(lambda: near(l)))

        def finish(l):
            with NS("cpair"):

                @pl.when(l == last)
                def _():
                    c_pairs(l, ndp - 2, nz).wait_recv()

                @pl.when(l != last)
                def _():
                    c_pairs(l, ndp, l).wait_recv()
                    rest_in(l).wait_recv()

            @pl.when(l != last)
            def _():
                with NS("group"):
                    accumulate(l, 0, ndp, False)

        both(k, finish)

    with NS("pairs"):
        c_pairs(last, ndp, last).wait_send()


def finishing(nz, ndp, blk_i, agrad_i, acc, a_v, cot_v, blk_o, agrad_o, wgrad_o, out_v, s, o_s):
    z, dp = lax.axis_index("cuts"), lax.axis_index("dp")
    last = last_plane(nz, z)
    first = 2 * (1 - lax.div(dp, 2))
    tok, heads = agrad_i.shape
    cols = acc.shape[1]
    scale = 1.0 / (nz * ndp)
    blk_copy = pltpu.make_async_copy(blk_i, blk_o, s.at[0])
    agrad_copy = pltpu.make_async_copy(agrad_i, agrad_o, s.at[1])
    blk_copy.start()
    agrad_copy.start()
    wide = 256 if heads % 256 == 0 else heads

    def out_copy(j):
        at = pl.ds(pl.multiple_of(j * wide, wide), wide)
        return pltpu.make_async_copy(out_v.at[at, :], wgrad_o.at[at, :], o_s.at[j])

    @pl.loop(0, heads // wide)
    def _(j):
        at = pl.ds(pl.multiple_of(j * wide, wide), wide)
        value = lax.dot_general(
            a_v[last, pl.ds(first, 2), :, at].reshape(2 * tok, wide),
            cot_v[last, pl.ds(first, 2)].reshape(2 * tok, cols),
            (((0,), (0,)), ((), ())),
            preferred_element_type=jnp.float32,
        )
        out_v[at, :] = scale * (acc[at, :] + value)
        out_copy(j).start()

    blk_copy.wait()
    agrad_copy.wait()

    @pl.loop(0, heads // wide)
    def _(j):
        out_copy(j).wait()


def fused_device(nz, ndp, attn_out, out_weight, residual, target, norm_gain):
    tok, heads = attn_out.shape
    half, width = residual.shape
    cols = width // ndp
    if cols != heads:
        return per_device(attn_out, out_weight, residual, target, norm_gain)
    chunk = 512 if width % 512 == 0 else 128
    chunks = width // chunk
    tiles = heads // 256 if heads % 256 == 0 else 1
    bf16, f32 = jnp.bfloat16, jnp.float32
    dma = pltpu.SemaphoreType.DMA
    in_vmem = pl.BlockSpec(memory_space=pltpu.VMEM)
    in_hbm = pl.BlockSpec(memory_space=pl.ANY)
    args = [attn_out, out_weight, residual, target, norm_gain.reshape(1, width)]
    args = [pltpu.with_memory_space_constraint(arg, pltpu.HBM) for arg in args]
    kept = pl.pallas_call(
        functools.partial(fused, nz, ndp, chunk),
        out_shape=(
            pltpu.VMEM((half, width), bf16),
            pltpu.VMEM((tok, heads), bf16),
            pltpu.VMEM((heads, cols), f32),
            pltpu.VMEM((nz, ndp, tok, heads), bf16),
            pltpu.VMEM((nz, ndp, 2, half, cols), bf16),
        ),
        in_specs=[in_hbm] * 5,
        out_specs=(in_vmem,) * 5,
        scratch_shapes=[
            pltpu.VMEM((heads, width), bf16),
            pltpu.VMEM((ndp, 2, half, cols), bf16),
            pltpu.VMEM((2, half, width), bf16),
            pltpu.VMEM((half, width), bf16),
            pltpu.VMEM((half, width), bf16),
            pltpu.VMEM((half, width), bf16),
            pltpu.VMEM((1, width), f32),
            dma((3,)), dma((chunks // (2 if chunks % 2 == 0 else 1),)), dma((1,)), dma((1,)),
            dma((nz,)), dma((nz,)), dma((nz, 2)), dma((nz,)), dma((nz,)), dma((nz,)), dma((nz,)),
            dma((1,)), dma((1,)), dma((1,)), dma((nz, ndp)), dma((nz,)), dma((nz + 1,)),
        ],
        compiler_params=pltpu.CompilerParams(
            collective_id=0, has_side_effects=True, vmem_limit_bytes=34 * 1000 * 1000
        ),
    )(*args)
    return pl.pallas_call(
        functools.partial(finishing, nz, ndp),
        out_shape=(
            jax.ShapeDtypeStruct((half, width), bf16),
            jax.ShapeDtypeStruct((tok, heads), bf16),
            jax.ShapeDtypeStruct((heads, cols), f32),
        ),
        in_specs=[in_vmem] * 5,
        out_specs=(in_hbm,) * 3,
        scratch_shapes=[pltpu.VMEM((heads, cols), f32), dma((2,)), dma((tiles,))],
        compiler_params=pltpu.CompilerParams(vmem_limit_bytes=16 * 1000 * 1000),
    )(*kept)


def solution(mesh):
    if mesh.shape["mp"] == 2 and mesh.shape["dp"] == 4 and mesh.shape["cuts"] > 1:
        body = functools.partial(fused_device, mesh.shape["cuts"], mesh.shape["dp"])
    else:
        body = per_device
    placed = (
        P(("cuts", "dp"), "mp"),
        P("mp", None),
        P(("cuts", "dp", "mp"), None),
        P(("cuts", "dp", "mp"), None),
        P(),
    )
    return jax.shard_map(
        body,
        mesh=mesh,
        in_specs=placed,
        out_specs=(P(("cuts", "dp", "mp"), None), P(("cuts", "dp"), "mp"), P("mp", "dp")),
        check_vma=False,
    )
```

```python
import functools

import jax
import jax.numpy as jnp
from jax import lax
from jax.experimental import pallas as pl
from jax.experimental.pallas import tpu as pltpu
from jax.sharding import PartitionSpec as P

epsilon = 1e-06


def norm_backward(stream, target, norm_gain):
    center = stream - jnp.mean(stream, axis=1, keepdims=True)
    inv_std = lax.rsqrt(jnp.mean(center * center, axis=1, keepdims=True) + epsilon)
    normed = center * inv_std
    misfit = normed * norm_gain[None, :] - target.astype(jnp.float32)
    gain_err = misfit * norm_gain[None, :]
    bracket = (
        gain_err
        - jnp.mean(gain_err, axis=1, keepdims=True)
        - normed * jnp.mean(gain_err * normed, axis=1, keepdims=True)
    )
    return (inv_std * bracket).astype(jnp.bfloat16)


def per_device(attn_out, out_weight, residual, target, norm_gain):
    tokens_dev = attn_out.shape[0]
    head_cols = attn_out.shape[1]
    replica_scale = 1.0 / (lax.axis_size("cuts") * lax.axis_size("dp"))
    summed = lax.psum_scatter(
        jnp.dot(attn_out, out_weight, preferred_element_type=jnp.float32).astype(jnp.bfloat16),
        "mp",
        scatter_dimension=0,
        tiled=True,
    ).astype(jnp.float32)
    stream = summed + residual.astype(jnp.float32)
    block_out = stream.astype(jnp.bfloat16)
    cotangent = norm_backward(stream, target, norm_gain)
    portion = lax.all_gather(cotangent, "mp", axis=0, tiled=True)
    stored = portion
    act_acc = lax.dot_general(
        portion, out_weight, (((1,), (1,)), ((), ())), preferred_element_type=jnp.float32
    )
    collected, act_acc = (stored, act_acc)
    attn_grad = act_acc.astype(jnp.bfloat16)
    columns = lax.all_to_all(collected, "dp", split_axis=1, concat_axis=0, tiled=True)
    column_width = columns.shape[1]
    portion = lax.all_gather(attn_out, "dp", axis=0, tiled=True)
    blocks_in = portion.shape[0] // tokens_dev
    head_block = portion.reshape(blocks_in, tokens_dev, head_cols)
    column_part = columns.reshape(blocks_in, tokens_dev, column_width)
    shares = (
        jnp.einsum("bti,btj->bij", head_block, column_part, preferred_element_type=jnp.float32)
        * replica_scale
    )
    rounded = lax.optimization_barrier(shares.astype(jnp.bfloat16))
    grad_block = jnp.sum(rounded.astype(jnp.float32), axis=0)
    weight_grad = lax.psum(grad_block.astype(jnp.bfloat16), "cuts").astype(jnp.float32)
    return (block_out, attn_grad, weight_grad)


NS = jax.named_scope
HEAD = 3
MESH = pl.DeviceIdType.MESH


def remote(src, dst, send_sem, recv_sem, **where):
    return pltpu.make_async_remote_copy(
        src_ref=src, dst_ref=dst, send_sem=send_sem, recv_sem=recv_sem, device_id=where, device_id_type=MESH
    )


def last_plane(nz, z):
    return jnp.where(2 * z < nz - 1, nz - 1, 0)


def fused(
    nz, ndp, chunk, attn_h, w_h, res_h, tgt_h, gain_h, blk_v, agrad_v, acc, a_v, cot_v,
    w_v, rows_v, part, part_in, res_v, tgt_v, gain_v,
    near_s, ready_s, ld_s, w_s, p_s, p_r, up_s, dn_s, az_r, pl_s, fx_r, fy_r, pl_r, cp_s, cq_s, cq_r, c_r, ce_s, ce_r,
):
    z, dp, m = lax.axis_index("cuts"), lax.axis_index("dp"), lax.axis_index("mp")
    other = 1 - m
    px, py = lax.rem(dp, 2), lax.div(dp, 2)
    xn, yn, dg = 2 * py + 1 - px, 2 * (1 - py) + px, 2 * (1 - py) + 1 - px
    peers = (dp, xn, yn, dg)
    tok, heads = attn_h.shape
    half, width = res_h.shape
    cols = width // ndp
    chunks = width // chunk
    per_load = 2 if chunks % 2 == 0 else 1
    last = last_plane(nz, z)
    has_up, has_down = z + 1 < nz, z >= 1

    a_load = pltpu.make_async_copy(attn_h, a_v.at[z, dp], ld_s.at[0])
    loads = [
        pltpu.make_async_copy(res_h, res_v, ld_s.at[1]),
        pltpu.make_async_copy(tgt_h, tgt_v, ld_s.at[1]),
        pltpu.make_async_copy(gain_h, gain_v, ld_s.at[2]),
    ]
    a_load.start()

    def w_load(c):
        at = pl.ds(pl.multiple_of(c * per_load * chunk, chunk), per_load * chunk)
        return pltpu.make_async_copy(w_h.at[:, at], w_v.at[:, at], w_s.at[c])

    is_end = (z == 0) | (z == nz - 1)
    barrier = pltpu.get_barrier_semaphore()
    pl.when(has_up)(lambda: pl.semaphore_signal(barrier, inc=1, device_id={"cuts": z + 1}, device_id_type=MESH))
    pl.when(has_down)(lambda: pl.semaphore_signal(barrier, inc=1, device_id={"cuts": z - 1}, device_id_type=MESH))
    pl.semaphore_signal(barrier, inc=1, device_id={"mp": other}, device_id_type=MESH)

    @pl.when(is_end)
    def _():
        for peer in (xn, yn):
            pl.semaphore_signal(barrier, inc=1, device_id={"dp": peer}, device_id_type=MESH)

    with NS("aload"):
        a_load.wait()
    with NS("barrier"):
        pl.semaphore_wait(barrier, jnp.where(is_end, 4, 3))

    def rows(h):
        return pl.ds(h * half, half)

    def piece(l, d, h):
        return a_v.at[l, d, rows(h)]

    def a_up(l, h):
        return remote(piece(l, dp, h), piece(l, dp, h), up_s.at[l], az_r.at[l, h], cuts=z + 1)

    def a_down(l, h):
        return remote(piece(l, dp, h), piece(l, dp, h), dn_s.at[l], az_r.at[l, h], cuts=z - 1)

    def a_x(l, h):
        return remote(piece(l, dp, h), piece(l, dp, h), pl_s.at[l], (fx_r if h == 0 else pl_r).at[l], dp=xn)

    def a_y(l, h):
        return remote(piece(l, dp, h), piece(l, dp, h), pl_s.at[l], (fy_r if h == 1 else pl_r).at[l], dp=yn)

    def first_x_in(l):
        return remote(piece(l, xn, 0), piece(l, xn, 0), pl_s.at[l], fx_r.at[l], dp=xn)

    def first_y_in(l):
        return remote(piece(l, yn, 1), piece(l, yn, 1), pl_s.at[l], fy_r.at[l], dp=yn)

    def r_y(l):
        return remote(piece(l, xn, 0), piece(l, xn, 0), pl_s.at[l], pl_r.at[l], dp=yn)

    def r_x(l):
        return remote(piece(l, yn, 1), piece(l, yn, 1), pl_s.at[l], pl_r.at[l], dp=xn)

    def rest_in(l):
        return remote(a_v.at[l, :2], a_v.at[l, :2], pl_s.at[l], pl_r.at[l], dp=xn)

    def sent_up(l):
        return remote(a_v.at[l, :3], a_v.at[l, :3], up_s.at[l], pl_r.at[l], cuts=z + 1)

    def sent_down(l):
        return remote(a_v.at[l, :3], a_v.at[l, :3], dn_s.at[l], pl_r.at[l], cuts=z - 1)

    def sent_plane(l):
        return remote(a_v.at[l, :3], a_v.at[l, :3], pl_s.at[l], pl_r.at[l], dp=xn)

    def c_up(l, d, src=None):
        return remote(cot_v.at[l, d, m] if src is None else src, cot_v.at[l, d, m], up_s.at[l], c_r.at[l, d], cuts=z + 1)

    def c_down(l, d, src=None):
        return remote(cot_v.at[l, d, m] if src is None else src, cot_v.at[l, d, m], dn_s.at[l], c_r.at[l, d], cuts=z - 1)

    def c_pair(l, d, group):
        return remote(cot_v.at[l, d, m], cot_v.at[l, d, m], ce_s.at[l], ce_r.at[group], mp=other)

    def c_pairs(l, count, group):
        blocks = cot_v.at[l, :count, other]
        return remote(blocks, blocks, ce_s.at[l], ce_r.at[group], mp=other)

    def both(k, f):
        pl.when(z - k >= 0)(lambda: f(z - k))
        pl.when(z + k < nz)(lambda: f(z + k))

    def a_hop(k, h):
        if k >= nz:
            return

        @pl.when(z - k >= 0)
        def _():
            with NS("ahop"):
                a_up(z - k, h).wait_recv()
            pl.when(has_up)(lambda: a_up(z - k, h).start())

        @pl.when(z + k < nz)
        def _():
            with NS("ahop"):
                a_down(z + k, h).wait_recv()
            pl.when(has_down)(lambda: a_down(z + k, h).start())

    def a_plane(l):
        a_x(l, 0).start()
        a_y(l, 1).start()
        a_x(l, 1).start()
        a_y(l, 0).start()

    def relay(l):
        with NS("relay"):
            first_x_in(l).wait_recv()
        r_y(l).start()
        with NS("relay"):
            first_y_in(l).wait_recv()
        r_x(l).start()

    for h in range(2):
        pl.when(has_up)(lambda: a_up(z, h).start())
        pl.when(has_down)(lambda: a_down(z, h).start())
    for c in range(chunks // per_load):
        w_load(c).start()
    for load in loads:
        load.start()

    @pl.when(is_end)
    def _():
        a_plane(z)
        for peer in (xn, yn):
            pl.semaphore_signal(near_s, inc=1, device_id={"dp": peer}, device_id_type=MESH)
        with NS("near_s"):
            pl.semaphore_wait(near_s, 2)

        @pl.when((z == 0) & (nz > 2))
        def _():
            pl.semaphore_signal(ready_s, inc=1, device_id={"cuts": z + 1}, device_id_type=MESH)

        @pl.when((z == nz - 1) & (nz > 3))
        def _():
            pl.semaphore_signal(ready_s, inc=1, device_id={"cuts": z - 1}, device_id_type=MESH)

    def a_middle():
        with NS("ready_s"):
            pl.semaphore_wait(ready_s, 1)
        a_plane(z)

    def p_send(c):
        at = pl.ds(pl.multiple_of(c * chunk, chunk), chunk)
        return remote(part.at[other, :, at], part_in.at[:, at], p_s.at[0], p_r.at[0], mp=other)

    @pl.loop(0, chunks)
    def _(c):
        at = pl.ds(pl.multiple_of(c * chunk, chunk), chunk)
        pl.when(lax.rem(c, per_load) == 0)(lambda: w_load(lax.div(c, per_load)).wait())
        pl.when(jnp.logical_not(is_end) & (c == min(HEAD, chunks - 1)))(a_middle)
        value = jnp.dot(a_v[z, dp], w_v[:, at], preferred_element_type=jnp.float32).astype(jnp.bfloat16)
        part[0, :, at] = value[:half]
        part[1, :, at] = value[half:]
        p_send(c).start()

    a_hop(1, 0)
    relay(z)
    with NS("loads"):
        pltpu.make_async_copy(part, part, ld_s.at[1]).wait()
        loads[2].wait()

    with NS("psend"):
        remote(part_in, part_in, p_s.at[0], p_r.at[0], mp=other).wait()

    step = 16
    gain = gain_v[...]

    @pl.loop(0, half // step)
    def _(i):
        at = pl.ds(pl.multiple_of(i * step, step), step)
        stream = (
            part[m, at, :].astype(jnp.float32) + part_in[at, :].astype(jnp.float32) + res_v[at, :].astype(jnp.float32)
        )
        blk_v[at, :] = stream.astype(jnp.bfloat16)
        center = stream - jnp.mean(stream, axis=1, keepdims=True)
        inv_std = lax.rsqrt(jnp.mean(center * center, axis=1, keepdims=True) + epsilon)
        normed = center * inv_std
        gain_err = (normed * gain - tgt_v[at, :].astype(jnp.float32)) * gain
        bracket = (
            gain_err
            - jnp.mean(gain_err, axis=1, keepdims=True)
            - normed * jnp.mean(gain_err * normed, axis=1, keepdims=True)
        )
        cot = (inv_std * bracket).astype(jnp.bfloat16)
        for d in range(ndp):
            rows_v[d, m, at, :] = cot[:, d * cols : (d + 1) * cols]

    def c_plane(k):
        return remote(rows_v.at[peers[k], m], cot_v.at[z, dp, m], cp_s.at[0], c_r.at[z, dp], dp=peers[k])

    def c_rows():
        return remote(rows_v.at[:, m], rows_v.at[:, m], cq_s.at[0], cq_r.at[0], mp=other)

    def c_rows_in():
        return remote(rows_v.at[:, other], rows_v.at[:, other], cq_s.at[0], cq_r.at[0], mp=other)

    own = rows_v.at[dp, m]
    pl.when(has_up)(lambda: c_up(z, dp, own).start())
    pl.when(has_down)(lambda: c_down(z, dp, own).start())
    for k in range(1, ndp):
        c_plane(k).start()
    c_rows().start()
    cot_v[z, dp, m] = rows_v[dp, m]

    a_hop(1, 1)
    both(1, a_plane)
    with NS("crows"):
        c_rows_in().wait_recv()
    cot_v[z, dp, other] = rows_v[dp, other]

    tile = 512 if heads % 512 == 0 else heads

    def attn_tile(j):
        at = slice(j * tile, (j + 1) * tile)
        total = jnp.zeros((tok, tile), jnp.float32)
        for d in range(ndp):
            total += lax.dot_general(
                rows_v[d].reshape(tok, cols), w_v[at, d * cols : (d + 1) * cols], (((1,), (1,)), ((), ())),
                preferred_element_type=jnp.float32,
            )
        agrad_v[:, at] = total.astype(jnp.bfloat16)

    def c_forward(l, j, up, down):
        pl.when(up)(lambda: c_up(l, peers[j]).start())
        pl.when(down)(lambda: c_down(l, peers[j]).start())
        c_pair(l, peers[j], l if j < 2 else jnp.where(l == last, nz, l)).start()

    tiles = heads // tile
    for j in range(tiles):
        attn_tile(j)
        if j < 2:
            a_hop(2, j)
    for h in range(tiles, 2):
        a_hop(2, h)
    both(2, a_plane)
    for k in range(1, ndp):
        with NS("cplane"):
            c_up(z, peers[k]).wait_recv()
        c_forward(z, k, has_up, has_down)

    wide = 256 if heads % 256 == 0 else heads

    def accumulate(l, first, count, fresh):
        @pl.loop(0, heads // wide)
        def _(j):
            at = pl.ds(pl.multiple_of(j * wide, wide), wide)
            value = lax.dot_general(
                a_v[l, pl.ds(first, count), :, at].reshape(count * tok, wide),
                cot_v[l, pl.ds(first, count)].reshape(count * tok, cols),
                (((0,), (0,)), ((), ())),
                preferred_element_type=jnp.float32,
            )
            acc[at, :] = value if fresh else acc[at, :] + value

    with NS("cpair0"):
        c_pairs(z, ndp - 1, z).wait_recv()
    with NS("aarr0"):
        rest_in(z).wait_recv()
    with NS("group0"):
        accumulate(z, 0, ndp, True)

    def drain():
        @pl.loop(0, nz)
        def _(l):
            pl.when(has_up & (l <= z))(lambda: sent_up(l).wait_send())
            pl.when(has_down & (l >= z))(lambda: sent_down(l).wait_send())
            sent_plane(l).wait_send()

            @pl.when((l != last) & (l != z))
            def _():
                c_pairs(l, ndp, l).wait_send()

        c_pairs(z, ndp - 1, z).wait_send()
        blocks = cot_v.at[z, : ndp - 1, m]
        remote(blocks, blocks, cp_s.at[0], c_r.at[z, dp], dp=xn).wait_send()
        c_rows().wait_send()

    both(1, relay)
    def near(l):
        c_pairs(l, 2, l).wait_recv()
        rest_in(l).wait_recv()
        with NS("near"):
            accumulate(l, 2 * py, 2, False)

    def finish(l):
        @pl.when(l == last)
        def _():
            c_pairs(l, ndp - 2, nz).wait_recv()

        @pl.when(l != last)
        def _():
            with NS("cpair"):
                c_pairs(l, ndp, l).wait_recv()
                rest_in(l).wait_recv()
            with NS("group"):
                accumulate(l, 0, ndp, False)

    for k in range(1, nz):
        if k == nz - 1:
            with NS("drain"):
                drain()
        for h in range(2):
            a_hop(k + 2, h)
        if k + 2 < nz:
            both(k + 2, a_plane)
        for j in range(ndp):

            @pl.when(z - k >= 0)
            def _():
                with NS("cup"):
                    c_up(z - k, peers[j]).wait_recv()
                c_forward(z - k, j, has_up, False)

            @pl.when(z + k < nz)
            def _():
                with NS("cdown"):
                    c_down(z + k, peers[j]).wait_recv()
                c_forward(z + k, j, False, has_down)

            if j == ndp - 2 and k + 1 < nz:
                both(k + 1, relay)
            if j == 1:
                both(k, lambda l: pl.when(is_end & (l == last))(lambda: near(l)))

        both(k, lambda l: pl.when(is_end)(lambda: finish(l)))
        if k == nz - 2:

            @pl.when(jnp.logical_not(is_end))
            def _():
                for i in range(1, nz - 1):
                    both(i, lambda l: pl.when(l == last)(lambda: near(l)))
                    both(i, finish)

    with NS("pairs"):
        c_pairs(last, ndp, last).wait_send()


def finishing(nz, ndp, blk_i, agrad_i, acc, a_v, cot_v, blk_o, agrad_o, wgrad_o, out_v, s, o_s):
    z, dp = lax.axis_index("cuts"), lax.axis_index("dp")
    last = last_plane(nz, z)
    first = 2 * (1 - lax.div(dp, 2))
    tok, heads = agrad_i.shape
    cols = acc.shape[1]
    scale = 1.0 / (nz * ndp)
    blk_copy = pltpu.make_async_copy(blk_i, blk_o, s.at[0])
    agrad_copy = pltpu.make_async_copy(agrad_i, agrad_o, s.at[1])
    blk_copy.start()
    agrad_copy.start()
    wide = 256 if heads % 256 == 0 else heads

    def out_copy(j):
        at = pl.ds(pl.multiple_of(j * wide, wide), wide)
        return pltpu.make_async_copy(out_v.at[at, :], wgrad_o.at[at, :], o_s.at[j])

    @pl.loop(0, heads // wide)
    def _(j):
        at = pl.ds(pl.multiple_of(j * wide, wide), wide)
        value = lax.dot_general(
            a_v[last, pl.ds(first, 2), :, at].reshape(2 * tok, wide),
            cot_v[last, pl.ds(first, 2)].reshape(2 * tok, cols),
            (((0,), (0,)), ((), ())),
            preferred_element_type=jnp.float32,
        )
        out_v[at, :] = scale * (acc[at, :] + value)
        out_copy(j).start()

    blk_copy.wait()
    agrad_copy.wait()

    @pl.loop(0, heads // wide)
    def _(j):
        out_copy(j).wait()


def fused_device(nz, ndp, attn_out, out_weight, residual, target, norm_gain):
    tok, heads = attn_out.shape
    half, width = residual.shape
    cols = width // ndp
    if cols != heads:
        return per_device(attn_out, out_weight, residual, target, norm_gain)
    chunk = 512 if width % 512 == 0 else 128
    chunks = width // chunk
    tiles = heads // 256 if heads % 256 == 0 else 1
    bf16, f32 = jnp.bfloat16, jnp.float32
    dma = pltpu.SemaphoreType.DMA
    in_vmem = pl.BlockSpec(memory_space=pltpu.VMEM)
    in_hbm = pl.BlockSpec(memory_space=pl.ANY)
    args = [attn_out, out_weight, residual, target, norm_gain.reshape(1, width)]
    args = [pltpu.with_memory_space_constraint(arg, pltpu.HBM) for arg in args]
    kept = pl.pallas_call(
        functools.partial(fused, nz, ndp, chunk),
        out_shape=(
            pltpu.VMEM((half, width), bf16),
            pltpu.VMEM((tok, heads), bf16),
            pltpu.VMEM((heads, cols), f32),
            pltpu.VMEM((nz, ndp, tok, heads), bf16),
            pltpu.VMEM((nz, ndp, 2, half, cols), bf16),
        ),
        in_specs=[in_hbm] * 5,
        out_specs=(in_vmem,) * 5,
        scratch_shapes=[
            pltpu.VMEM((heads, width), bf16),
            pltpu.VMEM((ndp, 2, half, cols), bf16),
            pltpu.VMEM((2, half, width), bf16),
            pltpu.VMEM((half, width), bf16),
            pltpu.VMEM((half, width), bf16),
            pltpu.VMEM((half, width), bf16),
            pltpu.VMEM((1, width), f32),
            pltpu.SemaphoreType.REGULAR, pltpu.SemaphoreType.REGULAR, dma((3,)), dma((chunks // (2 if chunks % 2 == 0 else 1),)), dma((1,)), dma((1,)),
            dma((nz,)), dma((nz,)), dma((nz, 2)), dma((nz,)), dma((nz,)), dma((nz,)), dma((nz,)),
            dma((1,)), dma((1,)), dma((1,)), dma((nz, ndp)), dma((nz,)), dma((nz + 1,)),
        ],
        compiler_params=pltpu.CompilerParams(
            collective_id=0, has_side_effects=True, vmem_limit_bytes=34 * 1000 * 1000
        ),
    )(*args)
    return pl.pallas_call(
        functools.partial(finishing, nz, ndp),
        out_shape=(
            jax.ShapeDtypeStruct((half, width), bf16),
            jax.ShapeDtypeStruct((tok, heads), bf16),
            jax.ShapeDtypeStruct((heads, cols), f32),
        ),
        in_specs=[in_vmem] * 5,
        out_specs=(in_hbm,) * 3,
        scratch_shapes=[pltpu.VMEM((heads, cols), f32), dma((2,)), dma((tiles,))],
        compiler_params=pltpu.CompilerParams(vmem_limit_bytes=16 * 1000 * 1000),
    )(*kept)


def solution(mesh):
    if mesh.shape["mp"] == 2 and mesh.shape["dp"] == 4 and 1 < mesh.shape["cuts"] < 5:
        body = functools.partial(fused_device, mesh.shape["cuts"], mesh.shape["dp"])
    else:
        body = per_device
    placed = (
        P(("cuts", "dp"), "mp"),
        P("mp", None),
        P(("cuts", "dp", "mp"), None),
        P(("cuts", "dp", "mp"), None),
        P(),
    )
    return jax.shard_map(
        body,
        mesh=mesh,
        in_specs=placed,
        out_specs=(P(("cuts", "dp", "mp"), None), P(("cuts", "dp"), "mp"), P("mp", "dp")),
        check_vma=False,
    )
```

```python
import functools

import jax
import jax.numpy as jnp
from jax import lax
from jax.experimental import pallas as pl
from jax.experimental.pallas import tpu as pltpu
from jax.sharding import PartitionSpec as P

epsilon = 1e-06


def norm_backward(stream, target, norm_gain):
    center = stream - jnp.mean(stream, axis=1, keepdims=True)
    inv_std = lax.rsqrt(jnp.mean(center * center, axis=1, keepdims=True) + epsilon)
    normed = center * inv_std
    misfit = normed * norm_gain[None, :] - target.astype(jnp.float32)
    gain_err = misfit * norm_gain[None, :]
    bracket = (
        gain_err
        - jnp.mean(gain_err, axis=1, keepdims=True)
        - normed * jnp.mean(gain_err * normed, axis=1, keepdims=True)
    )
    return (inv_std * bracket).astype(jnp.bfloat16)


def per_device(attn_out, out_weight, residual, target, norm_gain):
    tokens_dev = attn_out.shape[0]
    head_cols = attn_out.shape[1]
    replica_scale = 1.0 / (lax.axis_size("cuts") * lax.axis_size("dp"))
    summed = lax.psum_scatter(
        jnp.dot(attn_out, out_weight, preferred_element_type=jnp.float32).astype(jnp.bfloat16),
        "mp",
        scatter_dimension=0,
        tiled=True,
    ).astype(jnp.float32)
    stream = summed + residual.astype(jnp.float32)
    block_out = stream.astype(jnp.bfloat16)
    cotangent = norm_backward(stream, target, norm_gain)
    portion = lax.all_gather(cotangent, "mp", axis=0, tiled=True)
    stored = portion
    act_acc = lax.dot_general(
        portion, out_weight, (((1,), (1,)), ((), ())), preferred_element_type=jnp.float32
    )
    collected, act_acc = (stored, act_acc)
    attn_grad = act_acc.astype(jnp.bfloat16)
    columns = lax.all_to_all(collected, "dp", split_axis=1, concat_axis=0, tiled=True)
    column_width = columns.shape[1]
    portion = lax.all_gather(attn_out, "dp", axis=0, tiled=True)
    blocks_in = portion.shape[0] // tokens_dev
    head_block = portion.reshape(blocks_in, tokens_dev, head_cols)
    column_part = columns.reshape(blocks_in, tokens_dev, column_width)
    shares = (
        jnp.einsum("bti,btj->bij", head_block, column_part, preferred_element_type=jnp.float32)
        * replica_scale
    )
    rounded = lax.optimization_barrier(shares.astype(jnp.bfloat16))
    grad_block = jnp.sum(rounded.astype(jnp.float32), axis=0)
    weight_grad = lax.psum(grad_block.astype(jnp.bfloat16), "cuts").astype(jnp.float32)
    return (block_out, attn_grad, weight_grad)


NS = jax.named_scope
HEAD = 3
MESH = pl.DeviceIdType.MESH


def remote(src, dst, send_sem, recv_sem, **where):
    return pltpu.make_async_remote_copy(
        src_ref=src, dst_ref=dst, send_sem=send_sem, recv_sem=recv_sem, device_id=where, device_id_type=MESH
    )


def last_plane(nz, z):
    return jnp.where(2 * z < nz - 1, nz - 1, 0)


def fused(
    nz, ndp, chunk, attn_h, w_h, res_h, tgt_h, gain_h, blk_v, agrad_v, acc, a_v, cot_v,
    w_v, rows_v, part, part_in, res_v, tgt_v, gain_v,
    ready_s, above_s, ld_s, w_s, p_r, up_s, dn_s, az_r, pl_s, fx_r, fy_r, pl_r, cq_r, c_r, cx_r, ce_r,
):
    z, dp, m = lax.axis_index("cuts"), lax.axis_index("dp"), lax.axis_index("mp")
    other = 1 - m
    px, py = lax.rem(dp, 2), lax.div(dp, 2)
    xn, yn, dg = 2 * py + 1 - px, 2 * (1 - py) + px, 2 * (1 - py) + 1 - px
    peers = (dp, xn, yn, dg)
    tok, heads = attn_h.shape
    half, width = res_h.shape
    cols = width // ndp
    chunks = width // chunk
    per_load = 2 if chunks % 2 == 0 else 1
    last = last_plane(nz, z)
    has_up, has_down = z + 1 < nz, z >= 1

    a_load = pltpu.make_async_copy(attn_h, a_v.at[z, dp], ld_s.at[0])
    loads = [
        pltpu.make_async_copy(res_h, res_v, ld_s.at[1]),
        pltpu.make_async_copy(tgt_h, tgt_v, ld_s.at[1]),
        pltpu.make_async_copy(gain_h, gain_v, ld_s.at[2]),
    ]
    a_load.start()

    def w_load(c):
        at = pl.ds(pl.multiple_of(c * per_load * chunk, chunk), per_load * chunk)
        return pltpu.make_async_copy(w_h.at[:, at], w_v.at[:, at], w_s.at[c])

    is_end = (z == 0) | (z == nz - 1)
    second = (z == 1) if nz == 4 else (z < 0)
    third = (z == 2) if nz == 4 else (z < 0)
    barrier = pltpu.get_barrier_semaphore()
    pl.when(has_up)(lambda: pl.semaphore_signal(barrier, inc=1, device_id={"cuts": z + 1}, device_id_type=MESH))

    @pl.when(has_down & jnp.logical_not(third))
    def _():
        pl.semaphore_signal(barrier, inc=1, device_id={"cuts": z - 1}, device_id_type=MESH)

    pl.semaphore_signal(barrier, inc=1, device_id={"mp": other}, device_id_type=MESH)

    @pl.when(is_end)
    def _():
        for peer in (xn, yn):
            pl.semaphore_signal(barrier, inc=1, device_id={"dp": peer}, device_id_type=MESH)

    with NS("aload"):
        a_load.wait()
    with NS("barrier"):
        pl.semaphore_wait(barrier, jnp.where(is_end, 4, jnp.where(second, 2, 3)))

    def rows(h):
        return pl.ds(h * half, half)

    def piece(l, d, h):
        return a_v.at[l, d, rows(h)]

    def a_up(l, h):
        return remote(piece(l, dp, h), piece(l, dp, h), up_s.at[l], az_r.at[l, h], cuts=z + 1)

    def a_down(l, h):
        return remote(piece(l, dp, h), piece(l, dp, h), dn_s.at[l], az_r.at[l, h], cuts=z - 1)

    def a_x(l, h):
        return remote(piece(l, dp, h), piece(l, dp, h), pl_s.at[0], (fx_r if h == 0 else pl_r).at[l], dp=xn)

    def a_y(l, h):
        return remote(piece(l, dp, h), piece(l, dp, h), pl_s.at[0], (fy_r if h == 1 else pl_r).at[l], dp=yn)

    def first_x_in(l):
        return remote(piece(l, xn, 0), piece(l, xn, 0), pl_s.at[0], fx_r.at[l], dp=xn)

    def first_y_in(l):
        return remote(piece(l, yn, 1), piece(l, yn, 1), pl_s.at[0], fy_r.at[l], dp=yn)

    def r_y(l):
        return remote(piece(l, xn, 0), piece(l, xn, 0), pl_s.at[0], pl_r.at[l], dp=yn)

    def r_x(l):
        return remote(piece(l, yn, 1), piece(l, yn, 1), pl_s.at[0], pl_r.at[l], dp=xn)

    def rest_in(l):
        return remote(a_v.at[l, :2], a_v.at[l, :2], pl_s.at[0], pl_r.at[l], dp=xn)

    def sent_up(l):
        return remote(a_v.at[l, :3], a_v.at[l, :3], up_s.at[l], pl_r.at[l], cuts=z + 1)

    def sent_down(l):
        return remote(a_v.at[l, :3], a_v.at[l, :3], dn_s.at[l], pl_r.at[l], cuts=z - 1)

    def sent_plane():
        return remote(a_v.at[:, :3], a_v.at[:, :3], pl_s.at[0], pl_r.at[0], dp=xn)

    def c_up(l, d, src=None):
        return remote(cot_v.at[l, d, m] if src is None else src, cot_v.at[l, d, m], up_s.at[l], c_r.at[l, d], cuts=z + 1)

    def c_down(l, d, src=None):
        return remote(cot_v.at[l, d, m] if src is None else src, cot_v.at[l, d, m], dn_s.at[l], c_r.at[l, d], cuts=z - 1)

    def cut(i):
        return pl.ds(0, half - 16) if i == 0 else pl.ds(half - 16, 16)

    def c_cut(l, i, sem, to):
        block = cot_v.at[l, dg, m, cut(i)]
        return remote(block, block, sem, c_r.at[l, dg] if i == 0 else cx_r.at[0], cuts=to)

    def c_pair_cut(l, i):
        block = cot_v.at[l, dg, m, cut(i)]
        return remote(block, block, w_s.at[l], ce_r.at[nz], mp=other)

    def c_pair(l, d, group):
        return remote(cot_v.at[l, d, m], cot_v.at[l, d, m], w_s.at[l], ce_r.at[group], mp=other)

    def c_pairs(l, count, group):
        blocks = cot_v.at[l, :count, other]
        return remote(blocks, blocks, w_s.at[l], ce_r.at[group], mp=other)

    def both(k, f):
        pl.when(z - k >= 0)(lambda: f(z - k))
        pl.when(z + k < nz)(lambda: f(z + k))

    def a_hop(k, h):
        if k >= nz:
            return

        @pl.when(z - k >= 0)
        def _():
            with NS("ahop"):
                a_up(z - k, h).wait_recv()
            pl.when(has_up)(lambda: a_up(z - k, h).start())

        @pl.when(z + k < nz)
        def _():
            with NS("ahop"):
                a_down(z + k, h).wait_recv()
            pl.when(has_down)(lambda: a_down(z + k, h).start())

    def a_plane(l):
        a_x(l, 0).start()
        a_y(l, 1).start()
        a_x(l, 1).start()
        a_y(l, 0).start()

    def relay(l):
        with NS("relay"):
            first_x_in(l).wait_recv()
        r_y(l).start()
        with NS("relay"):
            first_y_in(l).wait_recv()
        r_x(l).start()

    for h in range(2):
        pl.when(has_up & jnp.logical_not(second))(lambda: a_up(z, h).start())
        pl.when(has_down)(lambda: a_down(z, h).start())

    @pl.when(third)
    def _():
        pl.semaphore_signal(above_s, inc=1, device_id={"cuts": z - 1}, device_id_type=MESH)

    def a_second():
        with NS("above_s"):
            pl.semaphore_wait(above_s, 1)
        for h in range(2):
            a_up(z, h).start()

    for c in range(chunks // per_load):
        w_load(c).start()
    for load in loads:
        load.start()

    @pl.when(is_end)
    def _():
        a_plane(z)
        for peer in (xn, yn):
            pl.semaphore_signal(ready_s, inc=1, device_id={"dp": peer}, device_id_type=MESH)
        with NS("near_s"):
            pl.semaphore_wait(ready_s, 2)

        @pl.when((z == 0) & (nz > 2))
        def _():
            pl.semaphore_signal(ready_s, inc=1, device_id={"cuts": z + 1}, device_id_type=MESH)

        @pl.when((z == nz - 1) & (nz > 3))
        def _():
            pl.semaphore_signal(ready_s, inc=1, device_id={"cuts": z - 1}, device_id_type=MESH)

    def a_middle():
        with NS("ready_s"):
            pl.semaphore_wait(ready_s, 1)
        a_plane(z)

    def p_send(c):
        at = pl.ds(pl.multiple_of(c * chunk, chunk), chunk)
        return remote(part.at[other, :, at], part_in.at[:, at], ld_s.at[0], p_r.at[0], mp=other)

    @pl.loop(0, chunks)
    def _(c):
        at = pl.ds(pl.multiple_of(c * chunk, chunk), chunk)
        pl.when(lax.rem(c, per_load) == 0)(lambda: w_load(lax.div(c, per_load)).wait())
        pl.when(second & (c == min(1, chunks - 1)))(a_second)
        pl.when(jnp.logical_not(is_end) & (c == min(HEAD, chunks - 1)))(a_middle)
        value = jnp.dot(a_v[z, dp], w_v[:, at], preferred_element_type=jnp.float32).astype(jnp.bfloat16)
        part[0, :, at] = value[:half]
        part[1, :, at] = value[half:]
        p_send(c).start()

    a_hop(1, 0)
    relay(z)
    with NS("loads"):
        pltpu.make_async_copy(part, part, ld_s.at[1]).wait()
        loads[2].wait()

    with NS("psend"):
        remote(part_in, part_in, ld_s.at[0], p_r.at[0], mp=other).wait()

    step = 16
    gain = gain_v[...]

    @pl.loop(0, half // step)
    def _(i):
        at = pl.ds(pl.multiple_of(i * step, step), step)
        stream = (
            part[m, at, :].astype(jnp.float32) + part_in[at, :].astype(jnp.float32) + res_v[at, :].astype(jnp.float32)
        )
        blk_v[at, :] = stream.astype(jnp.bfloat16)
        center = stream - jnp.mean(stream, axis=1, keepdims=True)
        inv_std = lax.rsqrt(jnp.mean(center * center, axis=1, keepdims=True) + epsilon)
        normed = center * inv_std
        gain_err = (normed * gain - tgt_v[at, :].astype(jnp.float32)) * gain
        bracket = (
            gain_err
            - jnp.mean(gain_err, axis=1, keepdims=True)
            - normed * jnp.mean(gain_err * normed, axis=1, keepdims=True)
        )
        cot = (inv_std * bracket).astype(jnp.bfloat16)
        for d in range(ndp):
            rows_v[d, m, at, :] = cot[:, d * cols : (d + 1) * cols]

    def c_plane(k):
        return remote(rows_v.at[peers[k], m], cot_v.at[z, dp, m], w_s.at[nz], c_r.at[z, dp], dp=peers[k])

    def c_rows():
        return remote(rows_v.at[:, m], rows_v.at[:, m], w_s.at[nz + 1], cq_r.at[0], mp=other)

    def c_rows_in():
        return remote(rows_v.at[:, other], rows_v.at[:, other], w_s.at[nz + 1], cq_r.at[0], mp=other)

    own = rows_v.at[dp, m]
    pl.when(has_up)(lambda: c_up(z, dp, own).start())
    pl.when(has_down)(lambda: c_down(z, dp, own).start())
    for k in range(1, ndp):
        c_plane(k).start()
    c_rows().start()
    cot_v[z, dp, m] = rows_v[dp, m]

    a_hop(1, 1)
    both(1, a_plane)
    with NS("crows"):
        c_rows_in().wait_recv()
    cot_v[z, dp, other] = rows_v[dp, other]

    tile = 512 if heads % 512 == 0 else heads

    def attn_tile(j):
        at = slice(j * tile, (j + 1) * tile)
        total = jnp.zeros((tok, tile), jnp.float32)
        for d in range(ndp):
            total += lax.dot_general(
                rows_v[d].reshape(tok, cols), w_v[at, d * cols : (d + 1) * cols], (((1,), (1,)), ((), ())),
                preferred_element_type=jnp.float32,
            )
        agrad_v[:, at] = total.astype(jnp.bfloat16)

    def c_forward(l, j, up, down, pieces=False):
        if pieces:
            for i in range(2):
                pl.when(up)(lambda: c_cut(l, i, up_s.at[l], z + 1).start())
                pl.when(down)(lambda: c_cut(l, i, dn_s.at[l], z - 1).start())
        else:
            pl.when(up)(lambda: c_up(l, peers[j]).start())
            pl.when(down)(lambda: c_down(l, peers[j]).start())
        c_pair(l, peers[j], l if j < 2 else jnp.where(l == last, nz, l)).start()

    tiles = heads // tile
    for j in range(tiles):
        attn_tile(j)
        if j < 2:
            a_hop(2, j)
    for h in range(tiles, 2):
        a_hop(2, h)
    both(2, a_plane)
    for k in range(1, ndp):
        with NS("cplane"):
            c_up(z, peers[k]).wait_recv()
        c_forward(z, k, has_up, has_down)

    wide = 256 if heads % 256 == 0 else heads

    def accumulate(l, first, count, fresh):
        @pl.loop(0, heads // wide)
        def _(j):
            at = pl.ds(pl.multiple_of(j * wide, wide), wide)
            value = lax.dot_general(
                a_v[l, pl.ds(first, count), :, at].reshape(count * tok, wide),
                cot_v[l, pl.ds(first, count)].reshape(count * tok, cols),
                (((0,), (0,)), ((), ())),
                preferred_element_type=jnp.float32,
            )
            acc[at, :] = value if fresh else acc[at, :] + value

    with NS("cpair0"):
        c_pairs(z, ndp - 1, z).wait_recv()
    with NS("aarr0"):
        rest_in(z).wait_recv()
    with NS("group0"):
        accumulate(z, 0, ndp, True)

    def drain():
        @pl.loop(0, nz)
        def _(l):
            pl.when(has_up & (l <= z))(lambda: sent_up(l).wait_send())
            pl.when(has_down & (l >= z))(lambda: sent_down(l).wait_send())

            @pl.when((l != last) & (l != z))
            def _():
                c_pairs(l, ndp, l).wait_send()

        sent_plane().wait_send()
        c_pairs(z, ndp - 1, z).wait_send()
        blocks = cot_v.at[z, : ndp - 1, m]
        remote(blocks, blocks, w_s.at[nz], c_r.at[z, dp], dp=xn).wait_send()
        c_rows().wait_send()

    both(1, relay)
    def near(l):
        c_pairs(l, 2, l).wait_recv()
        rest_in(l).wait_recv()
        with NS("near"):
            accumulate(l, 2 * py, 2, False)

    def finish(l):
        @pl.when(l == last)
        def _():
            c_pairs(l, ndp - 2, nz).wait_recv()

        @pl.when(l != last)
        def _():
            with NS("cpair"):
                c_pairs(l, ndp, l).wait_recv()
                rest_in(l).wait_recv()
            with NS("group"):
                accumulate(l, 0, ndp, False)

    for k in range(1, nz):
        if k == nz - 1:
            with NS("drain"):
                drain()
        for h in range(2):
            a_hop(k + 2, h)
        if k + 2 < nz:
            both(k + 2, a_plane)
        for j in range(ndp):
            pieces = k == nz - 2 and j == ndp - 1

            if k == nz - 1 and j == ndp - 1:

                @pl.when(is_end)
                def _():
                    for i in range(2):
                        with NS("cut"):
                            c_cut(last, i, up_s.at[last], z).wait_recv()
                        c_pair_cut(last, i).start()

                continue

            @pl.when(z - k >= 0)
            def _():
                with NS("cup"):
                    c_up(z - k, peers[j]).wait_recv()
                c_forward(z - k, j, has_up, False, pieces)

            @pl.when(z + k < nz)
            def _():
                with NS("cdown"):
                    c_down(z + k, peers[j]).wait_recv()
                c_forward(z + k, j, False, has_down, pieces)

            if j == ndp - 2 and k + 1 < nz:
                both(k + 1, relay)
            if j == 1:
                both(k, lambda l: pl.when(is_end & (l == last))(lambda: near(l)))

        both(k, lambda l: pl.when(is_end)(lambda: finish(l)))
        if k == nz - 2:

            @pl.when(jnp.logical_not(is_end))
            def _():
                for i in range(1, nz - 1):
                    both(i, lambda l: pl.when(l == last)(lambda: near(l)))
                    both(i, finish)

    with NS("pairs"):
        c_pairs(last, ndp, last).wait_send()


def finishing(nz, ndp, blk_i, agrad_i, acc, a_v, cot_v, blk_o, agrad_o, wgrad_o, out_v, s, o_s):
    z, dp = lax.axis_index("cuts"), lax.axis_index("dp")
    last = last_plane(nz, z)
    first = 2 * (1 - lax.div(dp, 2))
    tok, heads = agrad_i.shape
    cols = acc.shape[1]
    scale = 1.0 / (nz * ndp)
    blk_copy = pltpu.make_async_copy(blk_i, blk_o, s.at[0])
    agrad_copy = pltpu.make_async_copy(agrad_i, agrad_o, s.at[1])
    blk_copy.start()
    agrad_copy.start()
    wide = 256 if heads % 256 == 0 else heads

    def out_copy(j):
        at = pl.ds(pl.multiple_of(j * wide, wide), wide)
        return pltpu.make_async_copy(out_v.at[at, :], wgrad_o.at[at, :], o_s.at[j])

    @pl.loop(0, heads // wide)
    def _(j):
        at = pl.ds(pl.multiple_of(j * wide, wide), wide)
        value = lax.dot_general(
            a_v[last, pl.ds(first, 2), :, at].reshape(2 * tok, wide),
            cot_v[last, pl.ds(first, 2)].reshape(2 * tok, cols),
            (((0,), (0,)), ((), ())),
            preferred_element_type=jnp.float32,
        )
        out_v[at, :] = scale * (acc[at, :] + value)
        out_copy(j).start()

    blk_copy.wait()
    agrad_copy.wait()

    @pl.loop(0, heads // wide)
    def _(j):
        out_copy(j).wait()


def fused_device(nz, ndp, attn_out, out_weight, residual, target, norm_gain):
    tok, heads = attn_out.shape
    half, width = residual.shape
    cols = width // ndp
    if cols != heads:
        return per_device(attn_out, out_weight, residual, target, norm_gain)
    chunk = 512 if width % 512 == 0 else 128
    chunks = width // chunk
    tiles = heads // 256 if heads % 256 == 0 else 1
    bf16, f32 = jnp.bfloat16, jnp.float32
    dma = pltpu.SemaphoreType.DMA
    in_vmem = pl.BlockSpec(memory_space=pltpu.VMEM)
    in_hbm = pl.BlockSpec(memory_space=pl.ANY)
    args = [attn_out, out_weight, residual, target, norm_gain.reshape(1, width)]
    args = [pltpu.with_memory_space_constraint(arg, pltpu.HBM) for arg in args]
    kept = pl.pallas_call(
        functools.partial(fused, nz, ndp, chunk),
        out_shape=(
            pltpu.VMEM((half, width), bf16),
            pltpu.VMEM((tok, heads), bf16),
            pltpu.VMEM((heads, cols), f32),
            pltpu.VMEM((nz, ndp, tok, heads), bf16),
            pltpu.VMEM((nz, ndp, 2, half, cols), bf16),
        ),
        in_specs=[in_hbm] * 5,
        out_specs=(in_vmem,) * 5,
        scratch_shapes=[
            pltpu.VMEM((heads, width), bf16),
            pltpu.VMEM((ndp, 2, half, cols), bf16),
            pltpu.VMEM((2, half, width), bf16),
            pltpu.VMEM((half, width), bf16),
            pltpu.VMEM((half, width), bf16),
            pltpu.VMEM((half, width), bf16),
            pltpu.VMEM((1, width), f32),
            pltpu.SemaphoreType.REGULAR, pltpu.SemaphoreType.REGULAR, dma((3,)), dma((max(nz + 2, chunks // (2 if chunks % 2 == 0 else 1)),)), dma((1,)),
            dma((nz,)), dma((nz,)), dma((nz, 2)), dma((1,)), dma((nz,)), dma((nz,)), dma((nz,)),
            dma((1,)), dma((nz, ndp)), dma((1,)), dma((nz + 1,)),
        ],
        compiler_params=pltpu.CompilerParams(
            collective_id=0, has_side_effects=True, vmem_limit_bytes=34 * 1000 * 1000
        ),
    )(*args)
    return pl.pallas_call(
        functools.partial(finishing, nz, ndp),
        out_shape=(
            jax.ShapeDtypeStruct((half, width), bf16),
            jax.ShapeDtypeStruct((tok, heads), bf16),
            jax.ShapeDtypeStruct((heads, cols), f32),
        ),
        in_specs=[in_vmem] * 5,
        out_specs=(in_hbm,) * 3,
        scratch_shapes=[pltpu.VMEM((heads, cols), f32), dma((2,)), dma((tiles,))],
        compiler_params=pltpu.CompilerParams(vmem_limit_bytes=16 * 1000 * 1000),
    )(*kept)


def solution(mesh):
    if mesh.shape["mp"] == 2 and mesh.shape["dp"] == 4 and 2 < mesh.shape["cuts"] < 5:
        body = functools.partial(fused_device, mesh.shape["cuts"], mesh.shape["dp"])
    else:
        body = per_device
    placed = (
        P(("cuts", "dp"), "mp"),
        P("mp", None),
        P(("cuts", "dp", "mp"), None),
        P(("cuts", "dp", "mp"), None),
        P(),
    )
    return jax.shard_map(
        body,
        mesh=mesh,
        in_specs=placed,
        out_specs=(P(("cuts", "dp", "mp"), None), P(("cuts", "dp"), "mp"), P("mp", "dp")),
        check_vma=False,
    )
```

```python
import functools

import jax
import jax.numpy as jnp
from jax import lax
from jax.experimental import pallas as pl
from jax.experimental.pallas import tpu as pltpu
from jax.sharding import PartitionSpec as P

epsilon = 1e-06


def norm_backward(stream, target, norm_gain):
    center = stream - jnp.mean(stream, axis=1, keepdims=True)
    inv_std = lax.rsqrt(jnp.mean(center * center, axis=1, keepdims=True) + epsilon)
    normed = center * inv_std
    misfit = normed * norm_gain[None, :] - target.astype(jnp.float32)
    gain_err = misfit * norm_gain[None, :]
    bracket = (
        gain_err
        - jnp.mean(gain_err, axis=1, keepdims=True)
        - normed * jnp.mean(gain_err * normed, axis=1, keepdims=True)
    )
    return (inv_std * bracket).astype(jnp.bfloat16)


def per_device(attn_out, out_weight, residual, target, norm_gain):
    tokens_dev = attn_out.shape[0]
    head_cols = attn_out.shape[1]
    replica_scale = 1.0 / (lax.axis_size("cuts") * lax.axis_size("dp"))
    summed = lax.psum_scatter(
        jnp.dot(attn_out, out_weight, preferred_element_type=jnp.float32).astype(jnp.bfloat16),
        "mp",
        scatter_dimension=0,
        tiled=True,
    ).astype(jnp.float32)
    stream = summed + residual.astype(jnp.float32)
    block_out = stream.astype(jnp.bfloat16)
    cotangent = norm_backward(stream, target, norm_gain)
    portion = lax.all_gather(cotangent, "mp", axis=0, tiled=True)
    stored = portion
    act_acc = lax.dot_general(
        portion, out_weight, (((1,), (1,)), ((), ())), preferred_element_type=jnp.float32
    )
    collected, act_acc = (stored, act_acc)
    attn_grad = act_acc.astype(jnp.bfloat16)
    columns = lax.all_to_all(collected, "dp", split_axis=1, concat_axis=0, tiled=True)
    column_width = columns.shape[1]
    portion = lax.all_gather(attn_out, "dp", axis=0, tiled=True)
    blocks_in = portion.shape[0] // tokens_dev
    head_block = portion.reshape(blocks_in, tokens_dev, head_cols)
    column_part = columns.reshape(blocks_in, tokens_dev, column_width)
    shares = (
        jnp.einsum("bti,btj->bij", head_block, column_part, preferred_element_type=jnp.float32)
        * replica_scale
    )
    rounded = lax.optimization_barrier(shares.astype(jnp.bfloat16))
    grad_block = jnp.sum(rounded.astype(jnp.float32), axis=0)
    weight_grad = lax.psum(grad_block.astype(jnp.bfloat16), "cuts").astype(jnp.float32)
    return (block_out, attn_grad, weight_grad)


NS = jax.named_scope
HEAD = 3
MESH = pl.DeviceIdType.MESH


def remote(src, dst, send_sem, recv_sem, **where):
    return pltpu.make_async_remote_copy(
        src_ref=src, dst_ref=dst, send_sem=send_sem, recv_sem=recv_sem, device_id=where, device_id_type=MESH
    )


def last_plane(nz, z):
    return jnp.where(2 * z < nz - 1, nz - 1, 0)


def fused(nz, ndp, chunk, semaphores, *refs):
    pl.run_scoped(lambda *scoped: exchange(nz, ndp, chunk, *refs, *scoped), *semaphores)


def exchange(
    nz, ndp, chunk, attn_h, w_h, res_h, tgt_h, gain_h, blk_v, agrad_v, acc, a_v, cot_v,
    w_v, rows_v, part, part_in, res_v, tgt_v, gain_v, slip_v,
    ready_s, above_s, ld_s, w_s, p_r, up_s, dn_s, az_r, pl_s, fx_r, fy_r, pl_r, cq_r, c_r, cx_r, ce_r, sz_r, sx_r,
):
    z, dp, m = lax.axis_index("cuts"), lax.axis_index("dp"), lax.axis_index("mp")
    other = 1 - m
    px, py = lax.rem(dp, 2), lax.div(dp, 2)
    xn, yn, dg = 2 * py + 1 - px, 2 * (1 - py) + px, 2 * (1 - py) + 1 - px
    peers = (dp, xn, yn, dg)
    tok, heads = attn_h.shape
    half, width = res_h.shape
    cols = width // ndp
    chunks = width // chunk
    per_load = 2 if chunks % 2 == 0 else 1
    last = last_plane(nz, z)
    has_up, has_down = z + 1 < nz, z >= 1

    a_load = pltpu.make_async_copy(attn_h, a_v.at[z, dp], ld_s.at[0])
    loads = [
        pltpu.make_async_copy(res_h, res_v, ld_s.at[1]),
        pltpu.make_async_copy(tgt_h, tgt_v, ld_s.at[1]),
        pltpu.make_async_copy(gain_h, gain_v, ld_s.at[2]),
    ]
    a_load.start()

    def w_load(c):
        at = pl.ds(pl.multiple_of(c * per_load * chunk, chunk), per_load * chunk)
        return pltpu.make_async_copy(w_h.at[:, at], w_v.at[:, at], w_s.at[c])

    is_end = (z == 0) | (z == nz - 1)
    second = (z == 1) if nz == 4 else (z < 0)
    third = (z == 2) if nz == 4 else (z < 0)
    barrier = pltpu.get_barrier_semaphore()
    pl.when(has_up)(lambda: pl.semaphore_signal(barrier, inc=1, device_id={"cuts": z + 1}, device_id_type=MESH))

    @pl.when(has_down & jnp.logical_not(third))
    def _():
        pl.semaphore_signal(barrier, inc=1, device_id={"cuts": z - 1}, device_id_type=MESH)

    pl.semaphore_signal(barrier, inc=1, device_id={"mp": other}, device_id_type=MESH)

    @pl.when(is_end)
    def _():
        for peer in (xn, yn):
            pl.semaphore_signal(barrier, inc=1, device_id={"dp": peer}, device_id_type=MESH)

    with NS("aload"):
        a_load.wait()
    with NS("barrier"):
        pl.semaphore_wait(barrier, jnp.where(is_end, 4, jnp.where(second, 2, 3)))

    def rows(h):
        return pl.ds(h * half, half)

    def piece(l, d, h):
        return a_v.at[l, d, rows(h)]

    def a_up(l, h):
        return remote(piece(l, dp, h), piece(l, dp, h), up_s.at[l], az_r.at[l, h], cuts=z + 1)

    def a_down(l, h):
        return remote(piece(l, dp, h), piece(l, dp, h), dn_s.at[l], az_r.at[l, h], cuts=z - 1)

    def a_x(l, h):
        return remote(piece(l, dp, h), piece(l, dp, h), pl_s.at[0], (fx_r if h == 0 else pl_r).at[l], dp=xn)

    def a_y(l, h):
        return remote(piece(l, dp, h), piece(l, dp, h), pl_s.at[0], (fy_r if h == 1 else pl_r).at[l], dp=yn)

    def first_x_in(l):
        return remote(piece(l, xn, 0), piece(l, xn, 0), pl_s.at[0], fx_r.at[l], dp=xn)

    def first_y_in(l):
        return remote(piece(l, yn, 1), piece(l, yn, 1), pl_s.at[0], fy_r.at[l], dp=yn)

    def r_y(l):
        return remote(piece(l, xn, 0), piece(l, xn, 0), pl_s.at[0], pl_r.at[l], dp=yn)

    def r_x(l):
        return remote(piece(l, yn, 1), piece(l, yn, 1), pl_s.at[0], pl_r.at[l], dp=xn)

    def rest_in(l):
        return remote(a_v.at[l, :2], a_v.at[l, :2], pl_s.at[0], pl_r.at[l], dp=xn)

    def sent_up(l):
        return remote(a_v.at[l, :3], a_v.at[l, :3], up_s.at[l], pl_r.at[l], cuts=z + 1)

    def sent_down(l):
        return remote(a_v.at[l, :3], a_v.at[l, :3], dn_s.at[l], pl_r.at[l], cuts=z - 1)

    def sent_plane():
        return remote(a_v.at[:, :3], a_v.at[:, :3], pl_s.at[0], pl_r.at[0], dp=xn)

    def c_up(l, d, src=None):
        return remote(cot_v.at[l, d, m] if src is None else src, cot_v.at[l, d, m], up_s.at[l], c_r.at[l, d], cuts=z + 1)

    def c_down(l, d, src=None):
        return remote(cot_v.at[l, d, m] if src is None else src, cot_v.at[l, d, m], dn_s.at[l], c_r.at[l, d], cuts=z - 1)

    def cut(i):
        return pl.ds(0, half - 8) if i == 0 else pl.ds(half - 8, 8)

    def c_cut(l, i, sem, to):
        block = cot_v.at[l, dg, m, cut(i)]
        return remote(block, block, sem, c_r.at[l, dg] if i == 0 else cx_r.at[0], cuts=to)

    def c_pair_cut(l, i):
        block = cot_v.at[l, dg, m, cut(i)]
        return remote(block, block, w_s.at[l], ce_r.at[nz], mp=other)

    def c_pair(l, d, group):
        return remote(cot_v.at[l, d, m], cot_v.at[l, d, m], w_s.at[l], ce_r.at[group], mp=other)

    def c_pairs(l, count, group):
        blocks = cot_v.at[l, :count, other]
        return remote(blocks, blocks, w_s.at[l], ce_r.at[group], mp=other)

    slip, part_cols = 8, heads // 2
    lean = (z == 1) & (dp == 0) if nz == 4 else z < 0
    lean_in = (z == 0) & (dp == 0) if nz == 4 else z < 0
    beside = (dp == 1) | (dp == 2)
    helps = (z == 1) & beside if nz == 4 else z < 0
    passes = (z == 0) & beside if nz == 4 else z < 0

    def like(count):
        return w_v.at[pl.ds(0, count), pl.ds(0, part_cols)]

    def slip_at(h):
        return a_v.at[1, 0, pl.ds((h + 1) * half - slip, slip), pl.ds(0, part_cols)]

    def a_lean(h):
        for block in (
            a_v.at[1, 0, pl.ds(h * half, half - slip)],
            a_v.at[1, 0, pl.ds((h + 1) * half - slip, slip), pl.ds(part_cols, heads - part_cols)],
        ):
            remote(block, block, dn_s.at[1], az_r.at[1, h], cuts=z - 1).start()

    def a_lean_in(h):
        rows_in = like(2 * half - slip)
        return remote(rows_in, rows_in, dn_s.at[1], az_r.at[1, h], cuts=z + 1)

    def slip_down(h):
        return remote(slip_at(h), slip_v, dn_s.at[1], sz_r.at[0], cuts=z - 1)

    def slip_in():
        return remote(slip_v, slip_v, dn_s.at[1], sz_r.at[0], cuts=z + 1)

    def slip_over(h):
        return remote(slip_v, slip_at(h), ld_s.at[1], sx_r.at[h], dp=0)

    def both(k, f):
        pl.when(z - k >= 0)(lambda: f(z - k))
        pl.when(z + k < nz)(lambda: f(z + k))

    def a_hop(k, h):
        if k >= nz:
            return

        @pl.when(z - k >= 0)
        def _():
            with NS("ahop"):
                a_up(z - k, h).wait_recv()
            pl.when(has_up)(lambda: a_up(z - k, h).start())

        @pl.when(z + k < nz)
        def _():
            with NS("ahop"):
                if k == 1:
                    pl.when(lean_in)(lambda: a_lean_in(h).wait_recv())
                    pl.when(jnp.logical_not(lean_in))(lambda: a_down(z + k, h).wait_recv())
                else:
                    a_down(z + k, h).wait_recv()
            pl.when(has_down)(lambda: a_down(z + k, h).start())

    def a_plane(l):
        a_x(l, 0).start()
        a_y(l, 1).start()
        a_x(l, 1).start()
        a_y(l, 0).start()

    def relay(l):
        with NS("relay"):
            first_x_in(l).wait_recv()
        r_y(l).start()
        with NS("relay"):
            first_y_in(l).wait_recv()
        r_x(l).start()

    for h in range(2):
        pl.when(has_up & jnp.logical_not(second))(lambda: a_up(z, h).start())
        pl.when(has_down & jnp.logical_not(lean))(lambda: a_down(z, h).start())
        pl.when(lean)(lambda: a_lean(h))

    @pl.when(third)
    def _():
        pl.semaphore_signal(above_s, inc=1, device_id={"cuts": z - 1}, device_id_type=MESH)

    def a_second():
        with NS("above_s"):
            pl.semaphore_wait(above_s, 1)
        for h in range(2):
            a_up(z, h).start()

    for c in range(chunks // per_load):
        w_load(c).start()
    for load in loads:
        load.start()

    @pl.when(is_end)
    def _():
        a_plane(z)
        for peer in (xn, yn):
            pl.semaphore_signal(ready_s, inc=1, device_id={"dp": peer}, device_id_type=MESH)
        with NS("near_s"):
            pl.semaphore_wait(ready_s, 2)

        @pl.when((z == 0) & (nz > 2))
        def _():
            pl.semaphore_signal(ready_s, inc=1, device_id={"cuts": z + 1}, device_id_type=MESH)

        @pl.when((z == nz - 1) & (nz > 3))
        def _():
            pl.semaphore_signal(ready_s, inc=1, device_id={"cuts": z - 1}, device_id_type=MESH)

    def a_middle():
        with NS("ready_s"):
            pl.semaphore_wait(ready_s, 1)
        a_plane(z)

    def p_send(c):
        at = pl.ds(pl.multiple_of(c * chunk, chunk), chunk)
        return remote(part.at[other, :, at], part_in.at[:, at], ld_s.at[0], p_r.at[0], mp=other)

    @pl.loop(0, chunks)
    def _(c):
        at = pl.ds(pl.multiple_of(c * chunk, chunk), chunk)
        pl.when(lax.rem(c, per_load) == 0)(lambda: w_load(lax.div(c, per_load)).wait())
        pl.when(second & (c == min(1, chunks - 1)))(a_second)
        pl.when(jnp.logical_not(is_end) & (c == min(HEAD, chunks - 1)))(a_middle)
        value = jnp.dot(a_v[z, dp], w_v[:, at], preferred_element_type=jnp.float32).astype(jnp.bfloat16)
        part[0, :, at] = value[:half]
        part[1, :, at] = value[half:]
        p_send(c).start()

    a_hop(1, 0)
    relay(z)
    pl.when(helps & (dp == 1))(lambda: slip_down(0).start())
    pl.when(helps & (dp == 2))(lambda: slip_down(1).start())
    with NS("loads"):
        pltpu.make_async_copy(part, part, ld_s.at[1]).wait()
        loads[2].wait()

    with NS("psend"):
        remote(part_in, part_in, ld_s.at[0], p_r.at[0], mp=other).wait()

    step = 16
    gain = gain_v[...]

    @pl.loop(0, half // step)
    def _(i):
        at = pl.ds(pl.multiple_of(i * step, step), step)
        stream = (
            part[m, at, :].astype(jnp.float32) + part_in[at, :].astype(jnp.float32) + res_v[at, :].astype(jnp.float32)
        )
        blk_v[at, :] = stream.astype(jnp.bfloat16)
        center = stream - jnp.mean(stream, axis=1, keepdims=True)
        inv_std = lax.rsqrt(jnp.mean(center * center, axis=1, keepdims=True) + epsilon)
        normed = center * inv_std
        gain_err = (normed * gain - tgt_v[at, :].astype(jnp.float32)) * gain
        bracket = (
            gain_err
            - jnp.mean(gain_err, axis=1, keepdims=True)
            - normed * jnp.mean(gain_err * normed, axis=1, keepdims=True)
        )
        cot = (inv_std * bracket).astype(jnp.bfloat16)
        for d in range(ndp):
            rows_v[d, m, at, :] = cot[:, d * cols : (d + 1) * cols]

    def c_plane(k):
        return remote(rows_v.at[peers[k], m], cot_v.at[z, dp, m], w_s.at[nz], c_r.at[z, dp], dp=peers[k])

    def c_rows():
        return remote(rows_v.at[:, m], rows_v.at[:, m], w_s.at[nz + 1], cq_r.at[0], mp=other)

    def c_rows_in():
        return remote(rows_v.at[:, other], rows_v.at[:, other], w_s.at[nz + 1], cq_r.at[0], mp=other)

    own = rows_v.at[dp, m]
    pl.when(has_up)(lambda: c_up(z, dp, own).start())
    pl.when(has_down)(lambda: c_down(z, dp, own).start())
    for k in range(1, ndp):
        c_plane(k).start()
    c_rows().start()
    cot_v[z, dp, m] = rows_v[dp, m]

    a_hop(1, 1)
    both(1, lambda l: pl.when(jnp.logical_not(lean_in | passes))(lambda: a_plane(l)))
    with NS("crows"):
        c_rows_in().wait_recv()
    cot_v[z, dp, other] = rows_v[dp, other]

    tile = 512 if heads % 512 == 0 else heads

    def attn_tile(j):
        at = slice(j * tile, (j + 1) * tile)
        total = jnp.zeros((tok, tile), jnp.float32)
        for d in range(ndp):
            total += lax.dot_general(
                rows_v[d].reshape(tok, cols), w_v[at, d * cols : (d + 1) * cols], (((1,), (1,)), ((), ())),
                preferred_element_type=jnp.float32,
            )
        agrad_v[:, at] = total.astype(jnp.bfloat16)

    def c_forward(l, j, up, down, pieces=False):
        if pieces:
            for i in range(2):
                pl.when(up)(lambda: c_cut(l, i, up_s.at[l], z + 1).start())
                pl.when(down)(lambda: c_cut(l, i, dn_s.at[l], z - 1).start())
        else:
            pl.when(up)(lambda: c_up(l, peers[j]).start())
            pl.when(down)(lambda: c_down(l, peers[j]).start())
        c_pair(l, peers[j], l if j < 2 else jnp.where(l == last, nz, l)).start()

    tiles = heads // tile
    for j in range(tiles):
        attn_tile(j)
        if j == min(1, tiles - 1):

            @pl.when(lean_in)
            def _():
                with NS("slip"):
                    for h in range(2):
                        slip_over(h).wait_recv()
                a_plane(1)

        if j < 2:
            a_hop(2, j)
        if j == 0:

            @pl.when(passes)
            def _():
                with NS("slip"):
                    slip_in().wait_recv()
                pl.when(dp == 1)(lambda: slip_over(0).start())
                pl.when(dp == 2)(lambda: slip_over(1).start())
                a_plane(1)

    for h in range(tiles, 2):
        a_hop(2, h)
    both(2, a_plane)
    for k in range(1, ndp):
        with NS("cplane"):
            c_up(z, peers[k]).wait_recv()
        c_forward(z, k, has_up, has_down)

    wide = 256 if heads % 256 == 0 else heads

    def accumulate(l, first, count, fresh):
        @pl.loop(0, heads // wide)
        def _(j):
            at = pl.ds(pl.multiple_of(j * wide, wide), wide)
            value = lax.dot_general(
                a_v[l, pl.ds(first, count), :, at].reshape(count * tok, wide),
                cot_v[l, pl.ds(first, count)].reshape(count * tok, cols),
                (((0,), (0,)), ((), ())),
                preferred_element_type=jnp.float32,
            )
            acc[at, :] = value if fresh else acc[at, :] + value

    with NS("cpair0"):
        c_pairs(z, ndp - 1, z).wait_recv()
    with NS("aarr0"):
        rest_in(z).wait_recv()
    with NS("group0"):
        accumulate(z, 0, ndp, True)

    def drain():
        @pl.loop(0, nz)
        def _(l):
            pl.when(has_up & (l <= z))(lambda: sent_up(l).wait_send())
            uneven = (lean | helps) & (l == 1)
            pl.when(has_down & (l >= z) & jnp.logical_not(uneven))(lambda: sent_down(l).wait_send())

            @pl.when((l != last) & (l != z))
            def _():
                c_pairs(l, ndp, l).wait_send()

        for it, count in ((lean, 12 * half - 2 * slip), (helps, 12 * half + slip)):
            pl.when(it)(lambda: remote(like(count), like(count), dn_s.at[1], sz_r.at[0], cuts=z - 1).wait_send())
        pl.when(passes)(lambda: slip_over(0).wait_send())
        sent_plane().wait_send()
        c_pairs(z, ndp - 1, z).wait_send()
        blocks = cot_v.at[z, : ndp - 1, m]
        remote(blocks, blocks, w_s.at[nz], c_r.at[z, dp], dp=xn).wait_send()
        c_rows().wait_send()

    both(1, relay)
    def near(l):
        c_pairs(l, 2, l).wait_recv()
        rest_in(l).wait_recv()
        with NS("near"):
            accumulate(l, 2 * py, 2, False)

    def finish(l):
        @pl.when(l == last)
        def _():
            c_pairs(l, ndp - 2, nz).wait_recv()

        @pl.when(l != last)
        def _():
            with NS("cpair"):
                c_pairs(l, ndp, l).wait_recv()
                rest_in(l).wait_recv()
            with NS("group"):
                accumulate(l, 0, ndp, False)

    for k in range(1, nz):
        if k == nz - 1:
            with NS("drain"):
                drain()
        for h in range(2):
            a_hop(k + 2, h)
        if k + 2 < nz:
            both(k + 2, a_plane)
        for j in range(ndp):
            pieces = k == nz - 2 and j == ndp - 1

            if k == nz - 1 and j == ndp - 1:

                @pl.when(is_end)
                def _():
                    for i in range(2):
                        with NS("cut"):
                            c_cut(last, i, up_s.at[last], z).wait_recv()
                        c_pair_cut(last, i).start()

                continue

            @pl.when(z - k >= 0)
            def _():
                with NS("cup"):
                    c_up(z - k, peers[j]).wait_recv()
                c_forward(z - k, j, has_up, False, pieces)

            @pl.when(z + k < nz)
            def _():
                with NS("cdown"):
                    c_down(z + k, peers[j]).wait_recv()
                c_forward(z + k, j, False, has_down, pieces)

            if j == ndp - 2 and k + 1 < nz:
                both(k + 1, relay)
            if j == 1:
                both(k, lambda l: pl.when(is_end & (l == last))(lambda: near(l)))

        both(k, lambda l: pl.when(is_end)(lambda: finish(l)))
        if k == nz - 2:

            @pl.when(jnp.logical_not(is_end))
            def _():
                for i in range(1, nz - 1):
                    both(i, lambda l: pl.when(l == last)(lambda: near(l)))
                    both(i, finish)

    with NS("pairs"):
        c_pairs(last, ndp, last).wait_send()


def finishing(nz, ndp, tiles, *refs):
    dma = pltpu.SemaphoreType.DMA
    pl.run_scoped(lambda s, o_s: write_out(nz, ndp, *refs, s, o_s), dma((2,)), dma((tiles,)))


def write_out(nz, ndp, blk_i, agrad_i, acc, a_v, cot_v, blk_o, agrad_o, wgrad_o, out_v, s, o_s):
    z, dp = lax.axis_index("cuts"), lax.axis_index("dp")
    last = last_plane(nz, z)
    first = 2 * (1 - lax.div(dp, 2))
    tok, heads = agrad_i.shape
    cols = acc.shape[1]
    scale = 1.0 / (nz * ndp)
    blk_copy = pltpu.make_async_copy(blk_i, blk_o, s.at[0])
    agrad_copy = pltpu.make_async_copy(agrad_i, agrad_o, s.at[1])
    blk_copy.start()
    agrad_copy.start()
    wide = 256 if heads % 256 == 0 else heads

    def out_copy(j):
        at = pl.ds(pl.multiple_of(j * wide, wide), wide)
        return pltpu.make_async_copy(out_v.at[at, :], wgrad_o.at[at, :], o_s.at[j])

    @pl.loop(0, heads // wide)
    def _(j):
        at = pl.ds(pl.multiple_of(j * wide, wide), wide)
        value = lax.dot_general(
            a_v[last, pl.ds(first, 2), :, at].reshape(2 * tok, wide),
            cot_v[last, pl.ds(first, 2)].reshape(2 * tok, cols),
            (((0,), (0,)), ((), ())),
            preferred_element_type=jnp.float32,
        )
        out_v[at, :] = scale * (acc[at, :] + value)
        out_copy(j).start()

    blk_copy.wait()
    agrad_copy.wait()

    @pl.loop(0, heads // wide)
    def _(j):
        out_copy(j).wait()


def fused_device(nz, ndp, attn_out, out_weight, residual, target, norm_gain):
    tok, heads = attn_out.shape
    half, width = residual.shape
    cols = width // ndp
    if cols != heads:
        return per_device(attn_out, out_weight, residual, target, norm_gain)
    chunk = 512 if width % 512 == 0 else 128
    chunks = width // chunk
    tiles = heads // 256 if heads % 256 == 0 else 1
    bf16, f32 = jnp.bfloat16, jnp.float32
    dma = pltpu.SemaphoreType.DMA
    in_vmem = pl.BlockSpec(memory_space=pltpu.VMEM)
    in_hbm = pl.BlockSpec(memory_space=pl.ANY)
    semaphores = (
        pltpu.SemaphoreType.REGULAR, pltpu.SemaphoreType.REGULAR, dma((3,)), dma((max(nz + 2, chunks // (2 if chunks % 2 == 0 else 1)),)), dma((1,)),
        dma((nz,)), dma((nz,)), dma((nz, 2)), dma((1,)), dma((nz,)), dma((nz,)), dma((nz,)),
        dma((1,)), dma((nz, ndp)), dma((1,)), dma((nz + 1,)), dma((1,)), dma((2,)),
    )
    args = [attn_out, out_weight, residual, target, norm_gain.reshape(1, width)]
    args = [pltpu.with_memory_space_constraint(arg, pltpu.HBM) for arg in args]
    kept = pl.pallas_call(
        functools.partial(fused, nz, ndp, chunk, semaphores),
        out_shape=(
            pltpu.VMEM((half, width), bf16),
            pltpu.VMEM((tok, heads), bf16),
            pltpu.VMEM((heads, cols), f32),
            pltpu.VMEM((nz, ndp, tok, heads), bf16),
            pltpu.VMEM((nz, ndp, 2, half, cols), bf16),
        ),
        in_specs=[in_hbm] * 5,
        out_specs=(in_vmem,) * 5,
        scratch_shapes=[
            pltpu.VMEM((heads, width), bf16),
            pltpu.VMEM((ndp, 2, half, cols), bf16),
            pltpu.VMEM((2, half, width), bf16),
            pltpu.VMEM((half, width), bf16),
            pltpu.VMEM((half, width), bf16),
            pltpu.VMEM((half, width), bf16),
            pltpu.VMEM((1, width), f32),
            pltpu.VMEM((8, heads // 2), bf16),
        ],
        compiler_params=pltpu.CompilerParams(
            collective_id=0, has_side_effects=True, vmem_limit_bytes=34 * 1000 * 1000
        ),
    )(*args)
    return pl.pallas_call(
        functools.partial(finishing, nz, ndp, tiles),
        out_shape=(
            jax.ShapeDtypeStruct((half, width), bf16),
            jax.ShapeDtypeStruct((tok, heads), bf16),
            jax.ShapeDtypeStruct((heads, cols), f32),
        ),
        in_specs=[in_vmem] * 5,
        out_specs=(in_hbm,) * 3,
        scratch_shapes=[pltpu.VMEM((heads, cols), f32)],
        compiler_params=pltpu.CompilerParams(vmem_limit_bytes=16 * 1000 * 1000),
    )(*kept)


def solution(mesh):
    if mesh.shape["mp"] == 2 and mesh.shape["dp"] == 4 and 2 < mesh.shape["cuts"] < 5:
        body = functools.partial(fused_device, mesh.shape["cuts"], mesh.shape["dp"])
    else:
        body = per_device
    placed = (
        P(("cuts", "dp"), "mp"),
        P("mp", None),
        P(("cuts", "dp", "mp"), None),
        P(("cuts", "dp", "mp"), None),
        P(),
    )
    return jax.shard_map(
        body,
        mesh=mesh,
        in_specs=placed,
        out_specs=(P(("cuts", "dp", "mp"), None), P(("cuts", "dp"), "mp"), P("mp", "dp")),
        check_vma=False,
    )
```
